32 devices in a mesh: row: 2 (over x), col: 16 (over z, y, core).
Axes of the slice: x: 2, y: 2, z: 4, core: 2. Of those that a mesh axis runs over, the one named last changes fastest.
Arguments:
- tokens: bfloat16 [64, 128, 1024], P('row', 'col'), may hold values from -6 to 6
- shifts: int32 [2], replicated, may hold values from 0 to 15
- qkv_weight: bfloat16 [1024, 3, 1024], P('col', None, 'row'), may hold values from -0.1875 to 0.1875
- out_weight: bfloat16 [1024, 1024], P('row', 'col'), may hold values from -0.1875 to 0.1875
- up_weight: bfloat16 [1024, 4096], P('col', 'row'), may hold values from -0.1875 to 0.1875
- down_weight: bfloat16 [4096, 1024], P('row', 'col'), may hold values from -0.09375 to 0.09375
- qk_gain: float32 [1024], P('row'), may hold values from 0.5 to 1.5
- attn_rate: float32 [1024], replicated, may hold values from 0.1 to 0.6
- mlp_rate: float32 [1024], replicated, may hold values from 0.1 to 0.6
- hidden_gain: float32 [4096], P('row'), may hold values from 0.5 to 2
Outputs:
- sphere_out: bfloat16 [64, 128, 1024], P('row', 'col')
The draws below stay inside these ranges and needn't reach their ends.
Inputs may be any that keep to these rules, and one draw needn't show every extreme that they name: shifts[0] offsets the windows along rows, shifts[1] along columns.
All inputs are finite; a program needn't handle non-finite values.
Results may differ from the reference program's by a relative error of at most 0.012.
Values may be sent and summed in bfloat16 or wider, within the bound.
A program may use at most 128 MiB of HBM per device.

```python
import math
import jax
import jax.numpy as jnp
from jax import lax

D = 1024
H = 16
FF = 4096
HD = 64
WIN = 16
GRID_ROWS = 64
GRID_COLS = 128
N_ROW = 2


def levels(own_key, shape, shards, low, largest):
    def one(axis_at, parts):
        heights = jax.random.uniform(jax.random.fold_in(jax.random.fold_in(own_key, 6), axis_at), (parts,), jnp.float32, low / len(shards), largest / len(shards))
        return jnp.repeat(jnp.exp(heights), shape[axis_at] // parts).reshape((-1,) + (1,) * (len(shape) - axis_at - 1))

    loudness = one(*shards[0])
    for cut in shards[1:]:
        loudness = loudness * one(*cut)
    return loudness


def bell_draw(own_key, dims, scale, limit, shards=(), kind=jnp.bfloat16):
    drawn = scale * jax.random.normal(own_key, dims, jnp.float32)
    if shards:
        drawn = drawn * levels(own_key, dims, shards, -0.22, 0.18)
    return jnp.clip(drawn, -limit, limit).astype(kind)


def setup_inputs(seed: int = 0) -> dict:
    streams_of = jax.random.split(jax.random.key(seed), 11)
    return {
        "tokens": bell_draw(streams_of[0], (GRID_ROWS, GRID_COLS, D), 1.0, 6.0, ((0, 2), (1, 16))),
        "shifts": jax.random.randint(streams_of[1], (2,), 0, WIN).astype(jnp.int32),
        "qkv_weight": bell_draw(streams_of[2], (D, 3, D), D ** -0.5, 0.1875, ((0, 16), (2, 2))),
        "out_weight": bell_draw(streams_of[3], (D, D), D ** -0.5, 0.1875, ((0, 2), (1, 16))),
        "up_weight": bell_draw(streams_of[4], (D, FF), D ** -0.5, 0.1875, ((0, 16), (1, 2))),
        "down_weight": bell_draw(streams_of[5], (FF, D), FF ** -0.5, 0.09375, ((0, 2), (1, 16))),
        "qk_gain": jnp.clip(jnp.exp(math.log(1.5) - 1.0986123 * jax.random.uniform(streams_of[6], (D,), jnp.float32) ** levels(streams_of[6], (D,), ((0, 2),), -0.2, 0.2)), 0.5, 1.5),
        "attn_rate": jnp.clip(jnp.exp(jax.random.uniform(streams_of[7], (D,), jnp.float32, math.log(0.1), math.log(0.6))), 0.1, 0.6),
        "mlp_rate": jnp.clip(jnp.exp(jax.random.uniform(streams_of[8], (D,), jnp.float32, math.log(0.1), math.log(0.6))), 0.1, 0.6),
        "hidden_gain": jnp.clip(jnp.exp(math.log(2.0) - 1.3862944 * jax.random.uniform(streams_of[9], (FF,), jnp.float32) ** levels(streams_of[9], (FF,), ((0, 2),), -0.2, 0.2)), 0.5, 2.0),
    }


def to_sphere(vector):
    return vector * lax.rsqrt(lax.optimization_barrier(jnp.mean(vector * vector, axis=-1, keepdims=True)) + 1e-06)

def rounded(vector):
    return lax.optimization_barrier(vector.astype(jnp.bfloat16)).astype(jnp.float32)

def window_band(operands):
    query_band, key_band, value_band = operands
    scores = jnp.einsum('wqhd,wkhd->whqk', query_band.astype(jnp.float32), key_band.astype(jnp.float32)) / math.sqrt(HD)
    expo = jnp.exp(scores)
    weights = (expo / lax.optimization_barrier(jnp.sum(expo, axis=-1, keepdims=True))).astype(jnp.bfloat16)
    return jnp.einsum('whqk,wkhd->wqhd', weights.astype(jnp.float32), value_band.astype(jnp.float32)).astype(jnp.bfloat16)

def reference(tokens, shifts, qkv_weight, out_weight, up_weight, down_weight, qk_gain, attn_rate, mlp_rate, hidden_gain):
    grid_rows = tokens.shape[0]
    grid_cols = tokens.shape[1]
    token_count = grid_rows * grid_cols
    sphere = to_sphere(tokens.astype(jnp.float32)).reshape(token_count, D)
    sphere_bf = sphere.astype(jnp.bfloat16)
    projected = jnp.dot(sphere_bf, qkv_weight.reshape(D, 3 * D), preferred_element_type=jnp.float32)
    projected = projected.reshape(grid_rows, grid_cols, 3, H, HD)
    head_gain = qk_gain.reshape(H, HD)
    queries = (to_sphere(projected[:, :, 0]) * head_gain).astype(jnp.bfloat16)
    keys_sphere = (to_sphere(projected[:, :, 1]) * head_gain).astype(jnp.bfloat16)
    values = projected[:, :, 2].astype(jnp.bfloat16)
    shift_row = shifts[0]
    shift_col = shifts[1]

    def to_windows(field):
        rolled = jnp.roll(jnp.roll(field, -shift_row, axis=0), -shift_col, axis=1)
        rolled = rolled.reshape(grid_rows // WIN, WIN, grid_cols // WIN, WIN, H, HD)
        return rolled.transpose(0, 2, 1, 3, 4, 5).reshape(grid_rows // WIN, grid_cols // WIN, WIN * WIN, H, HD)
    attended = lax.map(window_band, (to_windows(queries), to_windows(keys_sphere), to_windows(values)))
    attended = attended.reshape(grid_rows // WIN, grid_cols // WIN, WIN, WIN, H, HD)
    attended = attended.transpose(0, 2, 1, 3, 4, 5).reshape(grid_rows, grid_cols, D)
    attended = jnp.roll(jnp.roll(attended, shift_row, axis=0), shift_col, axis=1).reshape(token_count, D)
    group_width = D // N_ROW
    attn_total = jnp.zeros((token_count, D), jnp.float32)
    for group_index in range(N_ROW):
        first = group_index * group_width
        attn_total = attn_total + rounded(jnp.dot(attended[:, first:first + group_width], out_weight[first:first + group_width], preferred_element_type=jnp.float32))
    mixed = to_sphere(sphere + attn_rate * (to_sphere(attn_total) - sphere))
    mixed_bf = mixed.astype(jnp.bfloat16)
    hidden_width = FF // N_ROW
    mlp_total = jnp.zeros((token_count, D), jnp.float32)
    for group_index in range(N_ROW):
        first = group_index * hidden_width
        raised = jnp.dot(mixed_bf, up_weight[:, first:first + hidden_width], preferred_element_type=jnp.float32) * hidden_gain[first:first + hidden_width]
        activated = jax.nn.gelu(raised, approximate=False).astype(jnp.bfloat16)
        mlp_total = mlp_total + rounded(jnp.dot(activated, down_weight[first:first + hidden_width], preferred_element_type=jnp.float32))
    sphere_out = to_sphere(mixed + mlp_rate * (to_sphere(mlp_total) - mixed))
    return sphere_out.astype(jnp.bfloat16).reshape(grid_rows, grid_cols, D)
```

```python
import functools
import math

import jax
import jax.numpy as jnp
from jax import lax
from jax.experimental import pallas as pl
from jax.experimental.pallas import tpu as pltpu
from jax.sharding import PartitionSpec as P

HD = 64
WIN = 16
LANES = 128
EPS = 1e-06
BF = jnp.bfloat16
F32 = jnp.float32
MESH = pl.DeviceIdType.MESH
VMEM = pl.BlockSpec(memory_space=pltpu.VMEM)
ANY = pl.BlockSpec(memory_space=pl.ANY)
SMEM = pl.BlockSpec(memory_space=pltpu.SMEM)
LAST = (((1,), (1,)), ((), ()))


def to_sphere(vector):
    return vector * lax.rsqrt(jnp.mean(vector * vector, axis=-1, keepdims=True) + EPS)


class Links:
    def __init__(self, n_row, n_col, send_sem, recv_sem):
        self.n_row, self.n_col, self.nz = n_row, n_col, n_col // 4
        self.send_sem, self.recv_sem = send_sem, recv_sem
        self.row, self.col = lax.axis_index("row"), lax.axis_index("col")
        self.z, self.y, self.core = self.col // 4, (self.col // 2) % 2, self.col % 2
        self.z_next = (self.row, self.at(self.z + 1, self.y, self.core))
        self.z_prev = (self.row, self.at(self.z - 1, self.y, self.core))
        self.y_peer = (self.row, self.at(self.z, 1 - self.y, self.core))
        self.core_peer = (self.row, self.at(self.z, self.y, 1 - self.core))
        self.after = (self.row, lax.rem(self.col + 1, n_col))
        self.before = (self.row, lax.rem(self.col + n_col - 1, n_col))
        self.started = []

    def at(self, z, y, core):
        return (lax.rem(z + 2 * self.nz, self.nz) * 2 + y) * 2 + core

    def other_row(self, r):
        return (lax.rem(self.row + r, self.n_row), self.col)

    def greet(self, more):
        peers = [self.z_next, self.z_prev, self.y_peer, self.core_peer, self.after, self.before]
        peers += more + [self.other_row(r) for r in range(1, self.n_row)]
        barrier = pltpu.get_barrier_semaphore()
        for peer in peers:
            pl.semaphore_signal(barrier, inc=1, device_id=peer, device_id_type=MESH)
        pl.semaphore_wait(barrier, len(peers))

    def send(self, src, dst, peer):
        index = len(self.started)
        copy = pltpu.make_async_remote_copy(
            src_ref=src,
            dst_ref=dst,
            send_sem=self.send_sem.at[index],
            recv_sem=self.recv_sem.at[index],
            device_id=peer,
            device_id_type=MESH,
        )
        copy.start()
        self.started.append(copy)
        return copy


class Ring:
    def __init__(self, links, full, depth, low, size, relief):
        self.links, self.full, self.depth, self.low, self.size = links, full, depth, low, size
        self.relief = relief and links.nz > 1
        self.z_copy, self.y_copy, self.core_copy = {}, {}, {}

    def block(self, z, y):
        owner = self.links.at(z, y, self.links.core)
        start = pl.multiple_of(owner * self.depth + self.low, self.size)
        return self.full.at[pl.ds(start, self.size)]

    def to_core(self, name, block):
        self.core_copy[name] = self.links.send(block, block, self.links.core_peer)

    def begin(self):
        links = self.links
        own = self.block(links.z, links.y)
        self.z_copy[0] = links.send(own, own, links.z_next)
        self.y_copy[0] = links.send(own, own, links.y_peer)
        self.to_core(("z", 0), own)

    def along(self, t):
        links = self.links
        self.z_copy[t - 1].wait_recv()
        block = self.block(links.z - t, links.y)
        if t < links.nz - 1:
            self.z_copy[t] = links.send(block, block, links.z_next)
        if not (self.relief and t == 1):
            self.y_copy[t] = links.send(block, block, links.y_peer)
        self.to_core(("z", t), block)

    def across(self, t):
        links = self.links
        block = self.block(links.z - t, 1 - links.y)
        if self.relief and t == 1:
            self.extra.wait_recv()
        else:
            self.y_copy[t].wait_recv()
            if self.relief and t == 0:
                self.extra = links.send(block, block, links.z_next)
        self.to_core(("y", t), block)

    def arrive(self, t):
        self.core_copy["z", t].wait_recv()
        self.core_copy["y", t].wait_recv()

    def arrive_all(self):
        for t in range(self.links.nz):
            self.arrive(t)


def layer_kernel(n_row, n_col, dims, *refs):
    local_rows, cols, depth, width, hidden = dims
    shifts, tok_in, q_in, o_in, u_in, d_in, gain, attn_rate, mlp_rate, hidden_gain, out = refs[:11]
    q_full, o_full, u_full, d_full, o_raw, d_raw, tok, sphere, piece = refs[11:20]
    strip, q_all, kv_all, back, part_send, part_recv, part_own = refs[20:27]
    mixed, mixed_all, active, down_send, down_recv, down_own = refs[27:33]
    local_sem, send_sem, recv_sem, kv_send, kv_recv, back_send, back_recv = refs[33:]

    links = Links(n_row, n_col, send_sem, recv_sem)
    row, col, nz = links.row, links.col, links.nz
    own = local_rows * cols
    rows = local_rows * n_row
    band = WIN * cols
    bands = rows // WIN
    per_window = WIN // cols
    share = depth // n_col
    seat = lax.rem(col, per_window)
    shift_row, shift_col = shifts[0], shifts[1]
    first = jnp.where(shift_col < cols, shift_col + cols, shift_col + cols - WIN)

    def mate(k):
        return (row, col - seat + lax.rem(seat + k, per_window))

    here = pl.ds(pl.multiple_of(col * share, share), share)
    local = [
        pltpu.make_async_copy(src, dst, local_sem.at[i])
        for i, (src, dst) in enumerate(
            [
                (q_in, q_full.at[here]),
                (tok_in, tok),
                (o_in, o_raw),
                (u_in, u_full.at[here]),
                (d_in, d_raw),
            ]
        )
    ]
    for copy in local:
        copy.start()
    links.greet([mate(k) for k in range(1, per_window)])

    half = share // 2
    q_a, q_b = [Ring(links, q_full, share, k * half, half, True) for k in range(2)]
    o_a = Ring(links, o_full, share, 0, share, False)
    u_a, u_b = [Ring(links, u_full, share, k * half, half, True) for k in range(2)]
    d_a, d_b = [Ring(links, d_full, share, k * half, half, True) for k in range(2)]

    local[0].wait()
    q_a.begin()
    q_b.begin()

    chunk = band
    steps = own // chunk
    local[1].wait()
    halo = []
    for i in range(steps):
        part = slice(i * chunk, (i + 1) * chunk)
        value = to_sphere(tok[part, :].astype(F32))
        sphere[part, :] = value
        piece[1, part, :] = value.astype(BF)
        halo.append(
            (
                links.send(piece.at[1, part], piece.at[2, part], links.before),
                links.send(piece.at[1, part], piece.at[0, part], links.after),
            )
        )

    eye = (
        lax.broadcasted_iota(jnp.int32, (share, share), 0)
        == lax.broadcasted_iota(jnp.int32, (share, share), 1)
    ).astype(F32).astype(BF)
    local[2].wait()
    o_full[here, :] = lax.dot_general(eye, o_raw[...], LAST, preferred_element_type=F32).astype(BF)
    o_a.begin()
    q_a.across(0)
    q_a.along(1)
    q_b.across(0)
    q_b.along(1)
    o_a.across(0)
    o_a.along(1)
    local[4].wait()
    d_full[here, :] = lax.dot_general(eye, d_raw[...], LAST, preferred_element_type=F32).astype(BF)

    bits = cols.bit_length() - 1

    def one_hot(length, row_step, column_step, per_piece):
        token = lax.broadcasted_iota(jnp.int32, (band, length), 0)
        source = lax.broadcasted_iota(jnp.int32, (band, length), 1)
        which = lax.shift_right_logical(source, per_piece.bit_length() - 1)
        source = source & (per_piece - 1)
        same_row = lax.shift_right_logical(source, bits) == (
            lax.shift_right_logical(token, bits) + row_step
        )
        same_column = which * cols + (source & (cols - 1)) == (token & (cols - 1)) + column_step
        return jnp.where(same_row & same_column, 1.0, 0.0).astype(BF)

    to_columns = one_hot(3 * band, 0, first, band)
    to_rows = one_hot(2 * band, shift_row, 0, 2 * band)
    to_home = one_hot(6 * band, WIN - shift_row, 2 * cols - first, 2 * band)

    q_a.along(2)
    q_b.along(2)
    local[3].wait()
    u_a.begin()
    u_b.begin()

    spread = []
    for i in range(steps):
        part = slice(i * chunk, (i + 1) * chunk)
        for copy in halo[i]:
            copy.wait_recv()
        near = jnp.concatenate([piece[k, part, :] for k in range(3)], axis=0)
        strip[0, part, :] = jnp.dot(to_columns, near, preferred_element_type=F32).astype(BF)
        spread.append(
            [
                links.send(strip.at[0, part], strip.at[r, part], links.other_row(r))
                for r in range(1, n_row)
            ]
        )
    q_a.across(1)
    q_b.across(1)
    for t in range(3, nz):
        q_a.along(t)
        q_b.along(t)
    for t in range(2, nz):
        q_a.across(t)
        q_b.across(t)
    o_a.along(2)
    o_a.across(1)

    for sent in spread:
        for copy in sent:
            copy.wait_recv()
    q_a.arrive_all()
    q_b.arrive_all()
    group = (lax.broadcasted_iota(jnp.int32, (LANES, LANES), 0) < HD) == (
        lax.broadcasted_iota(jnp.int32, (LANES, LANES), 1) < HD
    )
    averaging = jnp.where(group, 1.0 / HD, 0.0).astype(BF)

    def band_rows(b):
        return pl.ds(pl.multiple_of(b * band, band), band)

    def kv_copy(b, k):
        return pltpu.make_async_remote_copy(
            src_ref=kv_all.at[0, :, band_rows(b)],
            dst_ref=kv_all.at[k, :, band_rows(b)],
            send_sem=kv_send.at[b, k],
            recv_sem=kv_recv.at[b, k],
            device_id=mate(k),
            device_id_type=MESH,
        )

    def back_copy(b, k):
        return pltpu.make_async_remote_copy(
            src_ref=back.at[1, band_rows(b)],
            dst_ref=back.at[2 - 2 * k, band_rows(b)],
            send_sem=back_send.at[b, k],
            recv_sem=back_recv.at[b, k],
            device_id=(links.before, links.after)[k],
            device_id_type=MESH,
        )

    def block_of(b):
        slot = lax.rem(row - b // steps + n_row, n_row)
        return strip[slot, pl.ds(pl.multiple_of(lax.rem(b, steps) * band, band), band), :]

    def project(b, carry):
        near = jnp.concatenate([block_of(b), block_of(lax.rem(b + 1, bands))], axis=0)
        x = jnp.dot(to_rows, near, preferred_element_type=F32).astype(BF)
        for part in range(3):
            got = jnp.dot(
                x, q_full[:, part * width : (part + 1) * width], preferred_element_type=F32
            )
            if part == 2:
                kv_all[0, 1, band_rows(b), :] = got.astype(BF)
                continue
            for lo in range(0, width, LANES):
                cut = slice(lo, lo + LANES)
                one = got[:, cut]
                mean = jnp.dot((one * one).astype(BF), averaging, preferred_element_type=F32)
                scaled = one * lax.rsqrt(mean + EPS) * gain[:, cut]
                if part == 0:
                    q_all[band_rows(b), cut] = (scaled * (1.0 / math.sqrt(HD))).astype(BF)
                else:
                    kv_all[0, 0, band_rows(b), cut] = scaled.astype(BF)
        for k in range(1, per_window):
            kv_copy(b, k).start()
        return carry

    lax.fori_loop(0, bands, project, 0)
    u_a.across(0)
    u_a.along(1)
    u_b.across(0)
    u_b.along(1)
    for t in range(3, nz):
        o_a.along(t)
    for t in range(2, nz):
        o_a.across(t)

    lane = lax.broadcasted_iota(jnp.int32, (band, LANES), 1) < HD

    def attend(b, carry):
        for k in range(1, per_window):
            kv_copy(b, k).wait_recv()
        for lo in range(0, width, LANES):
            cut = slice(lo, lo + LANES)
            query = q_all[band_rows(b), cut].astype(F32)
            both = jnp.concatenate(
                [jnp.where(lane, query, 0.0), jnp.where(lane, 0.0, query)], axis=0
            ).astype(BF)
            keys = jnp.concatenate(
                [kv_all[k, 0, band_rows(b), cut] for k in range(per_window)], axis=0
            )
            values = jnp.concatenate(
                [kv_all[k, 1, band_rows(b), cut] for k in range(per_window)], axis=0
            )
            scores = lax.dot_general(both, keys, LAST, preferred_element_type=F32)
            expo = jnp.exp(scores)
            total = jnp.sum(expo, axis=-1, keepdims=True)
            got = jnp.dot(expo.astype(BF), values, preferred_element_type=F32) / total
            got = jnp.where(lane, got[:band], got[band:]).astype(BF)
            back[1, band_rows(b), cut] = got
        for k in range(2):
            back_copy(b, k).start()
        return carry

    middle = bands // 2
    lax.fori_loop(0, middle, attend, 0)
    u_a.across(1)
    u_b.across(1)
    if nz > 2:
        u_a.along(2)
        u_b.along(2)
    lax.fori_loop(middle, bands, attend, 0)
    for t in range(3, nz):
        u_a.along(t)
        u_b.along(t)
    d_a.begin()
    d_b.begin()
    for t in range(2, nz):
        u_a.across(t)
        u_b.across(t)
    d_a.across(0)
    d_b.across(0)
    d_a.along(1)
    d_b.along(1)

    def returned(b, carry):
        for k in range(2):
            back_copy(b, k).wait_recv()
        return carry

    lax.fori_loop(0, bands, returned, 0)
    o_a.arrive_all()

    def projected_out(owner, i):
        b = owner * steps + i
        earlier = lax.rem(b + bands - 1, bands)
        near = jnp.concatenate(
            [back[k, band_rows(at), :] for k in range(3) for at in (earlier, b)], axis=0
        )
        value = jnp.dot(to_home, near, preferred_element_type=F32).astype(BF)
        return lax.dot_general(value, o_full[...], LAST, preferred_element_type=F32)

    reduced = {}
    for i in range(steps):
        part = slice(i * chunk, (i + 1) * chunk)
        for r in range(1, n_row):
            part_send[r, part, :] = projected_out(lax.rem(row + r, n_row), i).astype(BF)
            reduced[i, r] = links.send(
                part_send.at[r, part], part_recv.at[r, part], links.other_row(r)
            )
    for i in range(steps):
        part_own[i * chunk : (i + 1) * chunk, :] = projected_out(row, i)

    d_a.across(1)
    d_b.across(1)
    if nz > 2:
        d_a.along(2)
        d_b.along(2)
    gathered = {}
    for i in range(steps):
        part = slice(i * chunk, (i + 1) * chunk)
        total = part_own[part, :]
        for r in range(1, n_row):
            reduced[i, r].wait_recv()
            total = total + part_recv[r, part, :].astype(F32)
        base = sphere[part, :]
        value = to_sphere(base + attn_rate[...] * (to_sphere(total) - base))
        mixed[part, :] = value
        mixed_all[0, part, :] = value.astype(BF)
        for r in range(1, n_row):
            gathered[i, r] = links.send(
                mixed_all.at[0, part], mixed_all.at[r, part], links.other_row(r)
            )
    for t in range(3, nz):
        d_a.along(t)
        d_b.along(t)

    u_a.arrive_all()
    u_b.arrive_all()
    tile = min(512, hidden)

    def raise_slot(r):
        def raise_tile(i, carry):
            cut = pl.ds(pl.multiple_of(i * tile, tile), tile)
            raised = jnp.dot(mixed_all[r], u_full[:, cut], preferred_element_type=F32)
            raised = raised * hidden_gain[:, cut]
            active[r, :, cut] = (
                0.5 * raised * (1.0 + lax.erf(raised * (1.0 / math.sqrt(2.0))))
            ).astype(BF)
            return carry

        lax.fori_loop(0, hidden // tile, raise_tile, 0)

    raise_slot(0)
    for t in range(2, nz):
        d_a.across(t)
        d_b.across(t)
    for r in range(1, n_row):
        for i in range(steps):
            gathered[i, r].wait_recv()
        raise_slot(r)

    span = 4 * share
    lowered = {}
    for t in range(nz):
        d_a.arrive(t)
        d_b.arrive(t)
        z = lax.rem(links.z - t + nz, nz)
        weight = d_full[pl.ds(pl.multiple_of(z * span, span), span), :]
        for r in list(range(1, n_row)) + [0]:
            got = lax.dot_general(active[r], weight, LAST, preferred_element_type=F32)
            if r == 0:
                down_own[z] = got
            else:
                down_send[r, z] = got.astype(BF)
                lowered[t, r] = links.send(
                    down_send.at[r, z], down_recv.at[r, z], links.other_row(n_row - r)
                )
    for copy in lowered.values():
        copy.wait_recv()
    for i in range(steps):
        part = slice(i * chunk, (i + 1) * chunk)
        pieces = []
        for z in range(nz):
            total = down_own[z, part, :]
            for r in range(1, n_row):
                total = total + down_recv[r, z, part, :].astype(F32)
            pieces.append(total)
        base = mixed[part, :]
        total = to_sphere(jnp.concatenate(pieces, axis=1))
        out[part, :] = to_sphere(base + mlp_rate[...] * (total - base)).astype(BF)

    for copy in links.started:
        copy.wait_send()

    def drain(b, carry):
        for k in range(1, per_window):
            kv_copy(b, k).wait_send()
        for k in range(2):
            back_copy(b, k).wait_send()
        return carry

    lax.fori_loop(0, bands, drain, 0)


def on_device(
    tokens,
    shifts,
    qkv_weight,
    out_weight,
    up_weight,
    down_weight,
    qk_gain,
    attn_rate,
    mlp_rate,
    hidden_gain,
):
    n_row = lax.axis_size("row")
    n_col = lax.axis_size("col")
    local_rows, cols, depth = tokens.shape
    width = qkv_weight.shape[2]
    hidden = up_weight.shape[1]
    own = local_rows * cols
    rows = local_rows * n_row
    count = rows * cols
    bands = rows // WIN
    per_window = WIN // cols
    share = depth // n_col
    nz = n_col // 4
    span = 4 * share
    steps = own // (WIN * cols)
    copies = 7 * 4 * nz + steps * (2 + 3 * (n_row - 1)) + nz * (n_row - 1)
    dma = pltpu.SemaphoreType.DMA
    result = pl.pallas_call(
        functools.partial(layer_kernel, n_row, n_col, (local_rows, cols, depth, width, hidden)),
        out_shape=jax.ShapeDtypeStruct((own, depth), BF),
        in_specs=[SMEM] + [ANY] * 5 + [VMEM] * 4,
        out_specs=VMEM,
        scratch_shapes=[
            pltpu.VMEM((depth, 3 * width), BF),
            pltpu.VMEM((depth, width), BF),
            pltpu.VMEM((depth, hidden), BF),
            pltpu.VMEM((depth, hidden), BF),
            pltpu.VMEM((width, share), BF),
            pltpu.VMEM((hidden, share), BF),
            pltpu.VMEM((own, depth), BF),
            pltpu.VMEM((own, depth), F32),
            pltpu.VMEM((3, own, depth), BF),
            pltpu.VMEM((n_row, own, depth), BF),
            pltpu.VMEM((count, width), BF),
            pltpu.VMEM((per_window, 2, count, width), BF),
            pltpu.VMEM((3, count, width), BF),
            pltpu.VMEM((n_row, own, depth), BF),
            pltpu.VMEM((n_row, own, depth), BF),
            pltpu.VMEM((own, depth), F32),
            pltpu.VMEM((own, depth), F32),
            pltpu.VMEM((n_row, own, depth), BF),
            pltpu.VMEM((n_row, own, hidden), BF),
            pltpu.VMEM((n_row, nz, own, span), BF),
            pltpu.VMEM((n_row, nz, own, span), BF),
            pltpu.VMEM((nz, own, span), F32),
            dma((5,)),
            dma((copies,)),
            dma((copies,)),
            dma((bands, per_window)),
            dma((bands, per_window)),
            dma((bands, 2)),
            dma((bands, 2)),
        ],
        compiler_params=pltpu.CompilerParams(
            collective_id=0, has_side_effects=True, vmem_limit_bytes=62 * 1024 * 1024
        ),
        name="layer",
    )(
        shifts,
        tokens.reshape(own, depth),
        qkv_weight.reshape(-1, 3 * width),
        out_weight,
        up_weight,
        down_weight,
        qk_gain.reshape(1, width),
        attn_rate.reshape(1, depth),
        mlp_rate.reshape(1, depth),
        hidden_gain.reshape(1, hidden),
    )
    return result.reshape(local_rows, cols, depth)


def solution(mesh):
    return jax.shard_map(
        on_device,
        mesh=mesh,
        in_specs=(
            P("row", "col", None),
            P(),
            P("col", None, "row"),
            P("row", "col"),
            P("col", "row"),
            P("row", "col"),
            P("row"),
            P(),
            P(),
            P("row"),
        ),
        out_specs=P("row", "col", None),
        check_vma=False,
    )
```

```python
import functools
import math

import jax
import jax.numpy as jnp
from jax import lax
from jax.experimental import pallas as pl
from jax.experimental.pallas import tpu as pltpu
from jax.sharding import PartitionSpec as P

HD = 64
WIN = 16
LANES = 128
EPS = 1e-06
BF = jnp.bfloat16
F32 = jnp.float32
MESH = pl.DeviceIdType.MESH
VMEM = pl.BlockSpec(memory_space=pltpu.VMEM)
ANY = pl.BlockSpec(memory_space=pl.ANY)
SMEM = pl.BlockSpec(memory_space=pltpu.SMEM)
LAST = (((1,), (1,)), ((), ()))


def to_sphere(vector):
    return vector * lax.rsqrt(jnp.mean(vector * vector, axis=-1, keepdims=True) + EPS)


class Links:
    def __init__(self, n_row, n_col, send_sem, recv_sem):
        self.n_row, self.n_col, self.nz = n_row, n_col, n_col // 4
        self.send_sem, self.recv_sem = send_sem, recv_sem
        self.row, self.col = lax.axis_index("row"), lax.axis_index("col")
        self.z, self.y, self.core = self.col // 4, (self.col // 2) % 2, self.col % 2
        self.z_next = (self.row, self.at(self.z + 1, self.y, self.core))
        self.z_prev = (self.row, self.at(self.z - 1, self.y, self.core))
        self.y_peer = (self.row, self.at(self.z, 1 - self.y, self.core))
        self.core_peer = (self.row, self.at(self.z, self.y, 1 - self.core))
        self.after = (self.row, lax.rem(self.col + 1, n_col))
        self.before = (self.row, lax.rem(self.col + n_col - 1, n_col))
        self.started = []

    def at(self, z, y, core):
        return (lax.rem(z + 2 * self.nz, self.nz) * 2 + y) * 2 + core

    def other_row(self, r):
        return (lax.rem(self.row + r, self.n_row), self.col)

    def greet(self, more):
        peers = [self.z_next, self.z_prev, self.y_peer, self.core_peer, self.after, self.before]
        peers += more + [self.other_row(r) for r in range(1, self.n_row)]
        barrier = pltpu.get_barrier_semaphore()
        for peer in peers:
            pl.semaphore_signal(barrier, inc=1, device_id=peer, device_id_type=MESH)
        pl.semaphore_wait(barrier, len(peers))

    def make(self, src, dst, peer):
        index = len(self.started)
        copy = pltpu.make_async_remote_copy(
            src_ref=src,
            dst_ref=dst,
            send_sem=self.send_sem.at[index],
            recv_sem=self.recv_sem.at[index],
            device_id=peer,
            device_id_type=MESH,
        )
        self.started.append(copy)
        return copy

    def send(self, src, dst, peer):
        copy = self.make(src, dst, peer)
        copy.start()
        return copy


class Ring:
    def __init__(self, links, full, depth, low, size, relief, rows=()):
        self.links, self.full, self.depth, self.low, self.size = links, full, depth, low, size
        self.relief = relief and links.nz > 1
        self.rows = rows
        self.z_copy, self.y_copy, self.core_copy, self.row_copy = {}, {}, {}, {}

    def place(self, z, y):
        owner = self.links.at(z, y, self.links.core)
        return pl.ds(pl.multiple_of(owner * self.depth + self.low, self.size), self.size)

    def block(self, z, y):
        return self.full.at[self.place(z, y)]

    def to_core(self, name, block):
        links = self.links
        self.core_copy[name] = links.send(block, block, links.core_peer)
        for r, there in self.rows:
            z = links.z - name[1]
            place = self.place(z, links.y if name[0] == "z" else 1 - links.y)
            self.row_copy[name, r] = links.send(block, there.at[place], links.other_row(r))

    def beyond(self):
        links = self.links
        for t in range(links.nz):
            for kind, y in (("z", links.y), ("y", 1 - links.y)):
                for r, there in self.rows:
                    self.row_copy[(kind, t), r].wait_recv()
                    block = there.at[self.place(links.z - t, y)]
                    self.core_copy[kind, t, r] = links.send(block, block, links.core_peer)

    def begin_z(self):
        own = self.block(self.links.z, self.links.y)
        self.z_copy[0] = self.links.send(own, own, self.links.z_next)
        self.to_core(("z", 0), own)

    def begin_y(self):
        own = self.block(self.links.z, self.links.y)
        self.y_copy[0] = self.links.send(own, own, self.links.y_peer)

    def begin(self):
        self.begin_z()
        self.begin_y()

    def along(self, t):
        links = self.links
        self.z_copy[t - 1].wait_recv()
        block = self.block(links.z - t, links.y)
        if t < links.nz - 1:
            self.z_copy[t] = links.send(block, block, links.z_next)
        if not (self.relief and t == 1):
            self.y_copy[t] = links.send(block, block, links.y_peer)
        self.to_core(("z", t), block)

    def across(self, t):
        links = self.links
        block = self.block(links.z - t, 1 - links.y)
        if self.relief and t == 1:
            self.extra.wait_recv()
        else:
            self.y_copy[t].wait_recv()
            if self.relief and t == 0:
                self.extra = links.send(block, block, links.z_next)
        self.to_core(("y", t), block)

    def arrive(self, t):
        self.core_copy["z", t].wait_recv()
        self.core_copy["y", t].wait_recv()

    def arrive_all(self):
        for copy in self.core_copy.values():
            copy.wait_recv()


def layer_kernel(n_row, n_col, dims, side, *refs):
    local_rows, cols, depth, width, hidden = dims
    shifts, tok_in, q_in, o_in, u_in, d_in, gain, attn_rate, mlp_rate, hidden_gain, out = refs[:11]
    q_full, o_all, u_full, d_full, tok, piece, sphere_all = refs[11:18]
    strip, q_all, kv_all, back, home_all = refs[18:23]
    mixed_all, active, down_send, down_recv, down_own = refs[23:28]
    local_sem, send_sem, recv_sem, kv_send, kv_recv, back_send, back_recv = refs[28:35]
    home_send, home_recv = refs[35:]

    links = Links(n_row, n_col, send_sem, recv_sem)
    row, col, nz = links.row, links.col, links.nz
    own = local_rows * cols
    rows = local_rows * n_row
    band = WIN * cols
    bands = rows // WIN
    per_window = WIN // cols
    share = depth // n_col
    seat = lax.rem(col, per_window)
    shift_row, shift_col = shifts[0], shifts[1]
    mine = 0 if side > 0 else 1
    first = shift_col if side > 0 else shift_col - cols

    def mate(k):
        return (row, col - seat + lax.rem(seat + k, per_window))

    here = pl.ds(pl.multiple_of(col * share, share), share)
    local = [
        pltpu.make_async_copy(src, dst, local_sem.at[i])
        for i, (src, dst) in enumerate(
            [(q_in.at[p], q_full.at[here, pl.ds(p * width, width)]) for p in range(3)]
            + [
                (tok_in, tok),
                (o_in, o_all.at[0, here]),
                (u_in, u_full.at[here]),
                (d_in, d_full.at[here]),
            ]
        )
    ]
    for copy in local:
        copy.start()
    source, target = (links.after, links.before) if side > 0 else (links.before, links.after)
    links.greet([mate(k) for k in range(1, per_window)])

    half = share // 2
    q_a, q_b = [Ring(links, q_full, share, k * half, half, k == 0) for k in range(2)]
    o_rows = [(r, o_all.at[r]) for r in range(1, n_row)]
    o_a = Ring(links, o_all.at[0], share, 0, share, False, o_rows)
    u_a, u_b = [Ring(links, u_full, share, k * half, half, k == 0) for k in range(2)]
    d_a, d_b = [Ring(links, d_full, share, k * half, half, k == 0) for k in range(2)]

    chunk = band
    steps = own // chunk
    local[3].wait()
    halo = []
    for i in range(steps):
        part = slice(i * chunk, (i + 1) * chunk)
        value = to_sphere(tok[part, :].astype(F32)).astype(BF)
        sphere_all[0, part, :] = value
        piece[mine, part, :] = value
        halo.append(links.send(piece.at[mine, part], piece.at[1 - mine, part], target))
    for copy in local[:3]:
        copy.wait()
    q_a.begin()
    q_b.begin()

    bits = cols.bit_length() - 1

    def one_hot(length, row_step, column_step, per_piece):
        token = lax.broadcasted_iota(jnp.int32, (band, length), 0)
        source = lax.broadcasted_iota(jnp.int32, (band, length), 1)
        which = lax.shift_right_logical(source, per_piece.bit_length() - 1)
        source = source & (per_piece - 1)
        same_row = lax.shift_right_logical(source, bits) == (
            lax.shift_right_logical(token, bits) + row_step
        )
        same_column = which * cols + (source & (cols - 1)) == (token & (cols - 1)) + column_step
        return jnp.where(same_row & same_column, 1.0, 0.0).astype(BF)

    to_columns = one_hot(2 * band, 0, first, band)
    to_rows = one_hot(2 * band, shift_row, 0, 2 * band)
    to_home = one_hot(4 * band, WIN - shift_row, cols - first, 2 * band)

    spread = [
        [
            links.make(
                strip.at[0, pl.ds(i * chunk, chunk)],
                strip.at[r, pl.ds(i * chunk, chunk)],
                links.other_row(r),
            )
            for r in range(1, n_row)
        ]
        for i in range(steps)
    ]

    def shift_columns():
        for i in range(steps):
            part = slice(i * chunk, (i + 1) * chunk)
            halo[i].wait_recv()
            near = jnp.concatenate([piece[k, part, :] for k in range(2)], axis=0)
            strip[0, part, :] = jnp.dot(to_columns, near, preferred_element_type=F32).astype(BF)
            for copy in spread[i]:
                copy.start()

    inside = links.core == (0 if side > 0 else 1)
    pl.when(inside)(shift_columns)
    for ring in (q_a, q_b):
        ring.across(0)
        ring.along(1)
    pl.when(jnp.logical_not(inside))(shift_columns)
    local[4].wait()
    o_a.begin()
    q_a.along(2)
    q_a.across(1)
    q_b.along(2)
    q_b.across(1)
    local[5].wait()
    u_a.begin_z()
    for ring in (q_a, q_b):
        for t in range(3, nz):
            ring.along(t)
        ring.across(2)
    u_a.begin_y()
    u_b.begin_z()
    around = [
        links.send(sphere_all.at[0], sphere_all.at[r], links.other_row(r))
        for r in range(1, n_row)
    ]
    o_a.along(1)
    o_a.across(0)
    for ring in (q_a, q_b):
        for t in range(3, nz):
            ring.across(t)
    u_b.begin_y()
    o_a.along(2)
    o_a.across(1)
    u_a.along(1)
    for sent in spread:
        for copy in sent:
            copy.wait_recv()
    q_a.arrive_all()
    q_b.arrive_all()
    group = (lax.broadcasted_iota(jnp.int32, (LANES, LANES), 0) < HD) == (
        lax.broadcasted_iota(jnp.int32, (LANES, LANES), 1) < HD
    )
    averaging = jnp.where(group, 1.0 / HD, 0.0).astype(BF)

    def band_rows(b):
        return pl.ds(pl.multiple_of(b * band, band), band)

    def kv_copy(b, k):
        return pltpu.make_async_remote_copy(
            src_ref=kv_all.at[0, :, band_rows(b)],
            dst_ref=kv_all.at[k, :, band_rows(b)],
            send_sem=kv_send.at[b, k],
            recv_sem=kv_recv.at[b, k],
            device_id=mate(k),
            device_id_type=MESH,
        )

    def back_copy(b):
        return pltpu.make_async_remote_copy(
            src_ref=back.at[1 - mine, band_rows(b)],
            dst_ref=back.at[mine, band_rows(b)],
            send_sem=back_send.at[b],
            recv_sem=back_recv.at[b],
            device_id=source,
            device_id_type=MESH,
        )

    def home_copy(b, r):
        return pltpu.make_async_remote_copy(
            src_ref=home_all.at[0, band_rows(b)],
            dst_ref=home_all.at[r, band_rows(b)],
            send_sem=home_send.at[b, r],
            recv_sem=home_recv.at[b, r],
            device_id=links.other_row(r),
            device_id_type=MESH,
        )

    def block_of(b):
        slot = lax.rem(row - b // steps + n_row, n_row)
        return strip[slot, pl.ds(pl.multiple_of(lax.rem(b, steps) * band, band), band), :]

    def project(b, carry):
        near = jnp.concatenate([block_of(b), block_of(lax.rem(b + 1, bands))], axis=0)
        x = jnp.dot(to_rows, near, preferred_element_type=F32).astype(BF)
        for part in range(3):
            got = jnp.dot(
                x, q_full[:, part * width : (part + 1) * width], preferred_element_type=F32
            )
            if part == 2:
                kv_all[0, 1, band_rows(b), :] = got.astype(BF)
                continue
            for lo in range(0, width, LANES):
                cut = slice(lo, lo + LANES)
                one = got[:, cut]
                mean = jnp.dot((one * one).astype(BF), averaging, preferred_element_type=F32)
                scaled = one * lax.rsqrt(mean + EPS) * gain[:, cut]
                if part == 0:
                    q_all[band_rows(b), cut] = (scaled * (1.0 / math.sqrt(HD))).astype(BF)
                else:
                    kv_all[0, 0, band_rows(b), cut] = scaled.astype(BF)
        for k in range(1, per_window):
            kv_copy(b, k).start()
        return carry

    lane = lax.broadcasted_iota(jnp.int32, (band, LANES), 1) < HD

    def attend(b, carry):
        for k in range(1, per_window):
            kv_copy(b, k).wait_recv()
        for lo in range(0, width, LANES):
            cut = slice(lo, lo + LANES)
            query = q_all[band_rows(b), cut].astype(F32)
            both = jnp.concatenate(
                [jnp.where(lane, query, 0.0), jnp.where(lane, 0.0, query)], axis=0
            ).astype(BF)
            keys = jnp.concatenate(
                [kv_all[k, 0, band_rows(b), cut] for k in range(per_window)], axis=0
            )
            values = jnp.concatenate(
                [kv_all[k, 1, band_rows(b), cut] for k in range(per_window)], axis=0
            )
            scores = lax.dot_general(both, keys, LAST, preferred_element_type=F32)
            expo = jnp.exp(scores)
            total = jnp.sum(expo, axis=-1, keepdims=True)
            got = jnp.dot(expo.astype(BF), values, preferred_element_type=F32) / total
            got = jnp.where(lane, got[:band], got[band:]).astype(BF)
            back[1 - mine, band_rows(b), cut] = got
        back_copy(b).start()
        return carry

    def project_attend(b, carry):
        project(b, 0)
        attend(b - 1, 0)
        return carry

    project(0, 0)
    u_b.along(1)
    u_a.across(0)
    u_b.across(0)
    lax.fori_loop(1, bands, project_attend, 0)
    attend(bands - 1, 0)
    u_a.along(2)
    u_b.along(2)
    for t in range(3, nz):
        o_a.along(t)
    o_a.across(2)
    local[6].wait()
    d_a.begin_z()

    def go_home(j, carry):
        b = lax.rem(j + 1, bands)

        @pl.when(j == 0)
        def _():
            back_copy(0).wait_recv()

        @pl.when(j < bands - 1)
        def _():
            back_copy(b).wait_recv()

        earlier = lax.rem(b + bands - 1, bands)
        near = jnp.concatenate(
            [back[k, band_rows(at), :] for k in range(2) for at in (earlier, b)], axis=0
        )
        home_all[0, band_rows(b), :] = jnp.dot(
            to_home, near, preferred_element_type=F32
        ).astype(BF)
        for r in range(1, n_row):
            home_copy(b, r).start()
        return carry

    lax.fori_loop(0, bands, go_home, 0)
    u_a.across(1)
    u_b.across(1)
    d_b.begin_z()
    for t in range(3, nz):
        o_a.across(t)
    d_a.begin_y()
    d_b.begin_y()
    for ring in (u_a, u_b):
        for t in range(3, nz):
            ring.along(t)
        ring.across(2)
    o_a.beyond()
    o_a.arrive_all()
    for copy in around:
        copy.wait_recv()

    def mix(j, carry):
        b = lax.rem(j + 1, bands)
        slot = lax.rem(row - b // steps + n_row, n_row)
        part = pl.ds(pl.multiple_of(lax.rem(b, steps) * chunk, chunk), chunk)
        total = None
        for r in range(n_row):
            if r > 0:
                home_copy(b, r).wait_recv()
            term = lax.dot_general(
                home_all[r, band_rows(b), :], o_all[r], LAST, preferred_element_type=F32
            )
            total = term if total is None else total + term
        base = sphere_all[slot, part, :].astype(F32)
        value = to_sphere(base + attn_rate[...] * (to_sphere(total) - base))
        mixed_all[slot, part, :] = value.astype(BF)
        return carry

    lax.fori_loop(0, bands, mix, 0)
    d_a.along(1)
    d_b.along(1)
    d_a.across(0)
    d_b.across(0)
    for ring in (u_a, u_b):
        for t in range(3, nz):
            ring.across(t)
    u_a.arrive_all()
    u_b.arrive_all()
    tile = min(512, hidden)

    def raise_slot(r):
        def raise_tile(i, carry):
            cut = pl.ds(pl.multiple_of(i * tile, tile), tile)
            raised = jnp.dot(mixed_all[r], u_full[:, cut], preferred_element_type=F32)
            raised = raised * hidden_gain[:, cut]
            active[r, :, cut] = (
                0.5 * raised * (1.0 + lax.erf(raised * (1.0 / math.sqrt(2.0))))
            ).astype(BF)
            return carry

        lax.fori_loop(0, hidden // tile, raise_tile, 0)

    raise_slot(0)
    for ring in (d_a, d_b):
        ring.along(2)
        ring.across(1)
    for r in range(1, n_row):
        raise_slot(r)
    for ring in (d_a, d_b):
        for t in range(3, nz):
            ring.along(t)
        ring.across(2)

    span = 4 * share
    lowered = {}
    for t in range(nz):
        for ring in (d_a, d_b):
            if t > 2:
                ring.across(t)
            ring.arrive(t)
        z = lax.rem(links.z - t + nz, nz)
        weight = d_full[pl.ds(pl.multiple_of(z * span, span), span), :]
        for r in list(range(1, n_row)) + [0]:
            got = lax.dot_general(active[r], weight, LAST, preferred_element_type=F32)
            if r == 0:
                down_own[z] = got
            else:
                down_send[r, z] = got.astype(BF)
                lowered[t, r] = links.send(
                    down_send.at[r, z], down_recv.at[r, z], links.other_row(n_row - r)
                )
    for copy in lowered.values():
        copy.wait_recv()
    for i in range(steps):
        part = slice(i * chunk, (i + 1) * chunk)
        pieces = []
        for z in range(nz):
            total = down_own[z, part, :]
            for r in range(1, n_row):
                total = total + down_recv[r, z, part, :].astype(F32)
            pieces.append(total)
        base = mixed_all[0, part, :].astype(F32)
        total = to_sphere(jnp.concatenate(pieces, axis=1))
        out[part, :] = to_sphere(base + mlp_rate[...] * (total - base)).astype(BF)

    for copy in links.started:
        copy.wait_send()

    def drain(b, carry):
        for k in range(1, per_window):
            kv_copy(b, k).wait_send()
        back_copy(b).wait_send()
        for r in range(1, n_row):
            home_copy(b, r).wait_send()
        return carry

    lax.fori_loop(0, bands, drain, 0)


def on_device(
    tokens,
    shifts,
    qkv_weight,
    out_weight,
    up_weight,
    down_weight,
    qk_gain,
    attn_rate,
    mlp_rate,
    hidden_gain,
):
    n_row = lax.axis_size("row")
    n_col = lax.axis_size("col")
    local_rows, cols, depth = tokens.shape
    width = qkv_weight.shape[2]
    hidden = up_weight.shape[1]
    own = local_rows * cols
    rows = local_rows * n_row
    count = rows * cols
    bands = rows // WIN
    per_window = WIN // cols
    share = depth // n_col
    nz = n_col // 4
    span = 4 * share
    steps = own // (WIN * cols)
    copies = 7 * 4 * nz + steps * n_row + (n_row - 1) * (5 * nz + 1)
    dma = pltpu.SemaphoreType.DMA
    dims = (local_rows, cols, depth, width, hidden)

    def layer(side, *operands):
        return pl.pallas_call(
        functools.partial(layer_kernel, n_row, n_col, dims, side),
        out_shape=jax.ShapeDtypeStruct((own, depth), BF),
        in_specs=[SMEM] + [ANY] * 5 + [VMEM] * 4,
        out_specs=VMEM,
        scratch_shapes=[
            pltpu.VMEM((depth, 3 * width), BF),
            pltpu.VMEM((n_row, depth, width), BF),
            pltpu.VMEM((depth, hidden), BF),
            pltpu.VMEM((depth, hidden), BF),
            pltpu.VMEM((own, depth), BF),
            pltpu.VMEM((2, own, depth), BF),
            pltpu.VMEM((n_row, own, depth), BF),
            pltpu.VMEM((n_row, own, depth), BF),
            pltpu.VMEM((count, width), BF),
            pltpu.VMEM((per_window, 2, count, width), BF),
            pltpu.VMEM((2, count, width), BF),
            pltpu.VMEM((n_row, count, width), BF),
            pltpu.VMEM((n_row, own, depth), BF),
            pltpu.VMEM((n_row, own, hidden), BF),
            pltpu.VMEM((n_row, nz, own, span), BF),
            pltpu.VMEM((n_row, nz, own, span), BF),
            pltpu.VMEM((nz, own, span), F32),
            dma((7,)),
            dma((copies,)),
            dma((copies,)),
            dma((bands, per_window)),
            dma((bands, per_window)),
            dma((bands,)),
            dma((bands,)),
            dma((bands, n_row)),
            dma((bands, n_row)),
        ],
        compiler_params=pltpu.CompilerParams(
            collective_id=0 if side > 0 else 1, has_side_effects=True, vmem_limit_bytes=62 * 1024 * 1024
        ),
        name="layer",
    )(*operands)

    result = lax.cond(
        shifts[1] < cols,
        functools.partial(layer, 1),
        functools.partial(layer, -1),
        shifts,
        tokens.reshape(own, depth),
        qkv_weight.transpose(1, 0, 2),
        out_weight.T,
        up_weight,
        down_weight.T,
        qk_gain.reshape(1, width),
        attn_rate.reshape(1, depth),
        mlp_rate.reshape(1, depth),
        hidden_gain.reshape(1, hidden),
    )
    return result.reshape(local_rows, cols, depth)


def solution(mesh):
    return jax.shard_map(
        on_device,
        mesh=mesh,
        in_specs=(
            P("row", "col", None),
            P(),
            P("col", None, "row"),
            P("row", "col"),
            P("col", "row"),
            P("row", "col"),
            P("row"),
            P(),
            P(),
            P("row"),
        ),
        out_specs=P("row", "col", None),
        check_vma=False,
    )
```

```python
import functools
import math

import jax
import jax.numpy as jnp
from jax import lax
from jax.experimental import pallas as pl
from jax.experimental.pallas import tpu as pltpu
from jax.sharding import PartitionSpec as P

HD = 64
WIN = 16
LANES = 128
EPS = 1e-06
BF = jnp.bfloat16
F32 = jnp.float32
MESH = pl.DeviceIdType.MESH
VMEM = pl.BlockSpec(memory_space=pltpu.VMEM)
ANY = pl.BlockSpec(memory_space=pl.ANY)
SMEM = pl.BlockSpec(memory_space=pltpu.SMEM)
LAST = (((1,), (1,)), ((), ()))


def to_sphere(vector):
    return vector * lax.rsqrt(jnp.mean(vector * vector, axis=-1, keepdims=True) + EPS)


class Links:
    def __init__(self, n_row, n_col, side, send_sem, recv_sem):
        self.side = side
        self.n_row, self.n_col, self.nz = n_row, n_col, n_col // 4
        self.send_sem, self.recv_sem = send_sem, recv_sem
        self.row, self.col = lax.axis_index("row"), lax.axis_index("col")
        self.z, self.y, self.core = self.col // 4, (self.col // 2) % 2, self.col % 2
        self.y_peer = (self.row, self.at(self.z, 1 - self.y, self.core))
        self.core_peer = (self.row, self.at(self.z, self.y, 1 - self.core))
        self.after = (self.row, lax.rem(self.col + 1, n_col))
        self.before = (self.row, lax.rem(self.col + n_col - 1, n_col))
        self.started = []

    def at(self, z, y, core):
        return (lax.rem(z + 2 * self.nz, self.nz) * 2 + y) * 2 + core

    def along(self, t):
        return (self.row, self.at(self.z + t, self.y, self.core))

    def turn(self, t):
        return t if self.side > 0 else (self.nz - t) % self.nz

    def other_row(self, r):
        return (lax.rem(self.row + r, self.n_row), self.col)

    def greet(self, more):
        peers = [self.y_peer, self.core_peer, self.after, self.before]
        peers += [self.along(t) for t in range(1, self.nz)]
        peers += more + [self.other_row(r) for r in range(1, self.n_row)]
        barrier = pltpu.get_barrier_semaphore()
        for peer in peers:
            pl.semaphore_signal(barrier, inc=1, device_id=peer, device_id_type=MESH)
        pl.semaphore_wait(barrier, len(peers))

    def make(self, src, dst, peer, when=None, landing=None):
        index = len(self.started)
        copy = pltpu.make_async_remote_copy(
            src_ref=src,
            dst_ref=dst,
            send_sem=self.send_sem.at[index],
            recv_sem=self.recv_sem.at[index if landing is None else landing],
            device_id=peer,
            device_id_type=MESH,
        )
        self.started.append((copy, when))
        return copy

    def send(self, src, dst, peer, when=None, landing=None):
        copy = self.make(src, dst, peer, when, landing)
        if when is None:
            copy.start()
        else:
            pl.when(when)(copy.start)
        return copy


class Spread:
    def __init__(self, links, full, depth, low, size, relief, relay, rows=()):
        self.links, self.full, self.depth, self.low, self.size = links, full, depth, low, size
        self.relief = relief and links.nz > 1
        self.relay = relay and links.nz > 2
        self.rows = rows
        self.z_copy, self.y_copy, self.core_copy, self.row_copy = {}, {}, {}, {}
        self.z_index, self.y_index = {}, {}
        for t in range(links.nz):
            when = None
            if self.relief and t in (1, links.nz - 1):
                when = links.z % 2 == (0 if t == 1 else 1)
            block = self.block(links.z - t, links.y)
            self.y_index[t] = len(links.started)
            self.y_copy[t] = links.make(block, block, links.y_peer, when)

    def place(self, z, y):
        owner = self.links.at(z, y, self.links.core)
        return pl.ds(pl.multiple_of(owner * self.depth + self.low, self.size), self.size)

    def block(self, z, y):
        return self.full.at[self.place(z, y)]

    def to_core(self, name, block):
        links = self.links
        self.core_copy[name] = links.send(block, block, links.core_peer)
        for r, there in self.rows:
            z = links.z - name[1]
            place = self.place(z, links.y if name[0] == "z" else 1 - links.y)
            self.row_copy[name, r] = links.send(block, there.at[place], links.other_row(r))

    def beyond(self):
        links = self.links
        for t in range(links.nz):
            for kind, y in (("z", links.y), ("y", 1 - links.y)):
                for r, there in self.rows:
                    self.row_copy[(kind, t), r].wait_recv()
                    block = there.at[self.place(links.z - t, y)]
                    self.core_copy[kind, t, r] = links.send(block, block, links.core_peer)

    def begin_z(self):
        links = self.links
        nz = links.nz
        own = self.block(links.z, links.y)
        for t in map(links.turn, sorted(range(1, nz), key=lambda t: -min(t, nz - t))):
            when = None
            if self.relay:
                when = {1: links.z != nz - 1, nz - 1: links.z != 0}.get(t)
            self.z_index[t] = len(links.started)
            self.z_copy[t] = links.send(own, own, links.along(t), when)
        self.to_core(("z", 0), own)

    def to_y(self, t):
        when = self.links.started[self.y_index[t]][1]
        if when is None:
            self.y_copy[t].start()
        else:
            pl.when(when)(self.y_copy[t].start)

    def begin_y(self):
        self.to_y(0)

    def begin(self):
        self.begin_z()
        self.begin_y()

    def along(self, t):
        links = self.links
        t = links.turn(t)
        nz = links.nz
        self.z_copy[t].wait_recv()
        block = self.block(links.z - t, links.y)
        if self.relay and t == 2:
            links.send(block, block, links.along(nz - 1), links.z == 1, self.z_index[1])
        if self.relay and t == nz - 2:
            links.send(block, block, links.along(1), links.z == nz - 2, self.z_index[nz - 1])
        self.to_y(t)
        self.to_core(("z", t), block)

    def across(self, t):
        t = self.links.turn(t)
        self.y_copy[t].wait_recv()
        self.to_core(("y", t), self.block(self.links.z - t, 1 - self.links.y))

    def pass_on(self):
        links = self.links
        self.across(0)
        if self.relief:
            block = self.block(links.z, 1 - links.y)
            even = links.z % 2 == 0
            partner = (links.row, links.at(links.z + 1 - 2 * (links.z % 2), links.y, links.core))
            landing = jnp.where(even, self.y_index[1], self.y_index[links.nz - 1])
            links.send(block, block, partner, None, landing)

    def arrive(self, t):
        t = self.links.turn(t)
        self.core_copy["z", t].wait_recv()
        self.core_copy["y", t].wait_recv()

    def arrive_all(self):
        for copy in self.core_copy.values():
            copy.wait_recv()


def layer_kernel(n_row, n_col, dims, side, *refs):
    local_rows, cols, depth, width, hidden = dims
    shifts, tok_in, q_in, o_in, u_in, d_in = refs[:6]
    vectors, out = refs[6:10], refs[10]
    q_full, o_all, u_full, d_full, tok, piece, sphere_all = refs[11:18]
    strip, q_all, kv_all, back, home_all = refs[18:23]
    mixed_all, active, down_send, down_recv, down_own = refs[23:28]
    local_sem, send_sem, recv_sem, kv_send, kv_recv, back_send, back_recv = refs[28:35]
    home_send, home_recv, gain, attn_rate, mlp_rate, hidden_gain = refs[35:]

    links = Links(n_row, n_col, side, send_sem, recv_sem)
    row, col, nz = links.row, links.col, links.nz
    own = local_rows * cols
    rows = local_rows * n_row
    band = WIN * cols
    bands = rows // WIN
    per_window = WIN // cols
    share = depth // n_col
    seat = lax.rem(col, per_window)
    shift_row, shift_col = shifts[0], shifts[1]
    mine = 0 if side > 0 else 1
    first = shift_col if side > 0 else shift_col - cols

    def mate(k):
        return (row, col - seat + lax.rem(seat + k, per_window))

    here = pl.ds(pl.multiple_of(col * share, share), share)
    local = [
        pltpu.make_async_copy(src, dst, local_sem.at[i])
        for i, (src, dst) in enumerate(
            [(q_in.at[p], q_full.at[here, pl.ds(p * width, width)]) for p in range(3)]
            + [
                (tok_in, tok),
                (o_in, o_all.at[0, here]),
                (u_in, u_full.at[here]),
                (d_in, d_full.at[here]),
            ]
            + list(zip(vectors, (gain, attn_rate, mlp_rate, hidden_gain)))
        )
    ]
    for copy in local:
        copy.start()
    source, target = (links.after, links.before) if side > 0 else (links.before, links.after)
    links.greet([mate(k) for k in range(1, per_window)])

    half = share // 2
    q_a = Spread(links, q_full, share, 0, half, True, False)
    q_b = Spread(links, q_full, share, half, half, False, True)
    o_rows = [(r, o_all.at[r]) for r in range(1, n_row)]
    o_a = Spread(links, o_all.at[0], share, 0, share, False, True, o_rows)
    u_a = Spread(links, u_full, share, 0, half, True, True)
    u_b = Spread(links, u_full, share, half, half, False, True)
    d_a = Spread(links, d_full, share, 0, half, False, True)
    d_b = Spread(links, d_full, share, half, half, True, True)

    chunk = band
    steps = own // chunk
    half_steps = steps // 2
    early, late = range(half_steps), range(half_steps, steps)
    halo = [
        links.make(
            piece.at[mine, pl.ds(i * chunk, chunk)],
            piece.at[1 - mine, pl.ds(i * chunk, chunk)],
            target,
        )
        for i in range(steps)
    ]
    bits = cols.bit_length() - 1

    def one_hot(length, row_step, column_step, per_piece):
        token = lax.broadcasted_iota(jnp.int32, (band, length), 0)
        source = lax.broadcasted_iota(jnp.int32, (band, length), 1)
        which = lax.shift_right_logical(source, per_piece.bit_length() - 1)
        source = source & (per_piece - 1)
        same_row = lax.shift_right_logical(source, bits) == (
            lax.shift_right_logical(token, bits) + row_step
        )
        same_column = which * cols + (source & (cols - 1)) == (token & (cols - 1)) + column_step
        return jnp.where(same_row & same_column, 1.0, 0.0).astype(BF)

    to_columns = one_hot(2 * band, 0, first, band)
    to_rows = one_hot(2 * band, shift_row, 0, 2 * band)
    to_home = one_hot(4 * band, WIN - shift_row, cols - first, 2 * band)

    spread = [
        [
            links.make(
                strip.at[0, pl.ds(i * chunk, chunk)],
                strip.at[r, pl.ds(i * chunk, chunk)],
                links.other_row(r),
            )
            for r in range(1, n_row)
        ]
        for i in range(steps)
    ]

    inside = links.core == (0 if side > 0 else 1)
    outside = jnp.logical_not(inside)

    def shift_columns(who, which):
        @pl.when(who)
        def _():
            for i in which:
                part = slice(i * chunk, (i + 1) * chunk)
                halo[i].wait_recv()
                near = jnp.concatenate([piece[k, part, :] for k in range(2)], axis=0)
                strip[0, part, :] = jnp.dot(
                    to_columns, near, preferred_element_type=F32
                ).astype(BF)
                for copy in spread[i]:
                    copy.start()

    group = (lax.broadcasted_iota(jnp.int32, (LANES, LANES), 0) < HD) == (
        lax.broadcasted_iota(jnp.int32, (LANES, LANES), 1) < HD
    )
    averaging = jnp.where(group, 1.0 / HD, 0.0).astype(BF)

    def band_rows(b):
        return pl.ds(pl.multiple_of(b * band, band), band)

    def kv_copy(b, k):
        return pltpu.make_async_remote_copy(
            src_ref=kv_all.at[0, :, band_rows(b)],
            dst_ref=kv_all.at[k, :, band_rows(b)],
            send_sem=kv_send.at[b, k],
            recv_sem=kv_recv.at[b, k],
            device_id=mate(k),
            device_id_type=MESH,
        )

    def back_copy(b):
        return pltpu.make_async_remote_copy(
            src_ref=back.at[1 - mine, band_rows(b)],
            dst_ref=back.at[mine, band_rows(b)],
            send_sem=back_send.at[b],
            recv_sem=back_recv.at[b],
            device_id=source,
            device_id_type=MESH,
        )

    def home_copy(b, r):
        return pltpu.make_async_remote_copy(
            src_ref=home_all.at[0, band_rows(b)],
            dst_ref=home_all.at[r, band_rows(b)],
            send_sem=home_send.at[b, r],
            recv_sem=home_recv.at[b, r],
            device_id=links.other_row(r),
            device_id_type=MESH,
        )

    def block_of(b):
        slot = lax.rem(row - b // steps + n_row, n_row)
        return strip[slot, pl.ds(pl.multiple_of(lax.rem(b, steps) * band, band), band), :]

    def project(b, carry):
        near = jnp.concatenate([block_of(b), block_of(lax.rem(b + 1, bands))], axis=0)
        x = jnp.dot(to_rows, near, preferred_element_type=F32).astype(BF)
        for part in range(3):
            got = jnp.dot(
                x, q_full[:, part * width : (part + 1) * width], preferred_element_type=F32
            )
            if part == 2:
                kv_all[0, 1, band_rows(b), :] = got.astype(BF)
                continue
            for lo in range(0, width, LANES):
                cut = slice(lo, lo + LANES)
                one = got[:, cut]
                mean = jnp.dot((one * one).astype(BF), averaging, preferred_element_type=F32)
                scaled = one * lax.rsqrt(mean + EPS) * gain[:, cut]
                if part == 0:
                    q_all[band_rows(b), cut] = (scaled * (1.0 / math.sqrt(HD))).astype(BF)
                else:
                    kv_all[0, 0, band_rows(b), cut] = scaled.astype(BF)
        for k in range(1, per_window):
            kv_copy(b, k).start()
        return carry

    lane = lax.broadcasted_iota(jnp.int32, (band, LANES), 1) < HD

    def attend(b, carry):
        for k in range(1, per_window):
            kv_copy(b, k).wait_recv()
        for lo in range(0, width, LANES):
            cut = slice(lo, lo + LANES)
            query = q_all[band_rows(b), cut].astype(F32)
            both = jnp.concatenate(
                [jnp.where(lane, query, 0.0), jnp.where(lane, 0.0, query)], axis=0
            ).astype(BF)
            keys = jnp.concatenate(
                [kv_all[k, 0, band_rows(b), cut] for k in range(per_window)], axis=0
            )
            values = jnp.concatenate(
                [kv_all[k, 1, band_rows(b), cut] for k in range(per_window)], axis=0
            )
            scores = lax.dot_general(both, keys, LAST, preferred_element_type=F32)
            expo = jnp.exp(scores)
            total = jnp.sum(expo, axis=-1, keepdims=True)
            got = jnp.dot(expo.astype(BF), values, preferred_element_type=F32) / total
            got = jnp.where(lane, got[:band], got[band:]).astype(BF)
            back[1 - mine, band_rows(b), cut] = got
        back_copy(b).start()
        return carry

    def project_attend(b, carry):
        project(b, 0)
        attend(b - 1, 0)
        return carry

    def go_home(j, carry):
        b = lax.rem(j + 1, bands)

        @pl.when(j == 0)
        def _():
            back_copy(0).wait_recv()

        @pl.when(j < bands - 1)
        def _():
            back_copy(b).wait_recv()

        earlier = lax.rem(b + bands - 1, bands)
        near = jnp.concatenate(
            [back[k, band_rows(at), :] for k in range(2) for at in (earlier, b)], axis=0
        )
        home_all[0, band_rows(b), :] = jnp.dot(
            to_home, near, preferred_element_type=F32
        ).astype(BF)
        for r in range(1, n_row):
            home_copy(b, r).start()
        return carry

    def mix(j, carry):
        b = lax.rem(j + 1, bands)
        slot = lax.rem(row - b // steps + n_row, n_row)
        part = pl.ds(pl.multiple_of(lax.rem(b, steps) * chunk, chunk), chunk)
        total = None
        for r in range(n_row):
            if r > 0:
                home_copy(b, r).wait_recv()
            term = lax.dot_general(
                home_all[r, band_rows(b), :], o_all[r], LAST, preferred_element_type=F32
            )
            total = term if total is None else total + term
        base = sphere_all[slot, part, :].astype(F32)
        value = to_sphere(base + attn_rate[...] * (to_sphere(total) - base))
        mixed_all[slot, part, :] = value.astype(BF)
        return carry

    tile = min(512, hidden)

    def raise_slot(r):
        def raise_tile(i, carry):
            cut = pl.ds(pl.multiple_of(i * tile, tile), tile)
            raised = jnp.dot(mixed_all[r], u_full[:, cut], preferred_element_type=F32)
            raised = raised * hidden_gain[:, cut]
            active[r, :, cut] = (
                0.5 * raised * (1.0 + lax.erf(raised * (1.0 / math.sqrt(2.0))))
            ).astype(BF)
            return carry

        lax.fori_loop(0, hidden // tile, raise_tile, 0)

    span = 4 * share
    lowered = []

    def lower_to(r, t):
        z = lax.rem(links.z - links.turn(t) + nz, nz)
        weight = d_full[pl.ds(pl.multiple_of(z * span, span), span), :]
        return z, lax.dot_general(active[r], weight, LAST, preferred_element_type=F32)

    def lower(t):
        d_a.arrive(t)
        d_b.arrive(t)
        for r in range(1, n_row):
            z, got = lower_to(r, t)
            down_send[r, z] = got.astype(BF)
            lowered.append(
                links.send(
                    down_send.at[r, z], down_recv.at[r, z], links.other_row(n_row - r)
                )
            )

    def lower_own(t):
        z, got = lower_to(0, t)
        down_own[z] = got

    def to_neighbour():
        for i in range(steps):
            part = slice(i * chunk, (i + 1) * chunk)
            value = to_sphere(tok[part, :].astype(F32)).astype(BF)
            sphere_all[0, part, :] = value
            piece[mine, part, :] = value

    for copy in local[:3]:
        copy.wait()
    q_b.begin_z()
    q_b.begin_y()
    local[5].wait()
    u_b.begin_y()
    local[4].wait()
    o_a.begin_y()
    local[3].wait()
    to_neighbour()
    for i in early:
        halo[i].start()
    around = [
        links.send(sphere_all.at[0], sphere_all.at[r], links.other_row(r))
        for r in range(1, n_row)
    ]
    shift_columns(inside, early)
    q_a.begin_z()
    q_a.begin_y()
    for i in late:
        halo[i].start()
    q_b.along(2)
    for copy in around:
        copy.wait_recv()
    o_a.begin_z()
    q_b.along(1)
    u_a.begin_y()
    shift_columns(outside, early)
    u_b.pass_on()
    q_b.pass_on()
    q_b.across(2)
    shift_columns(inside, late)
    q_a.pass_on()
    q_a.along(2)
    q_a.along(1)
    for t in range(3, nz):
        q_b.along(t)
    for t in range(3, nz):
        q_a.along(t)
    o_a.along(2)
    o_a.along(1)
    o_a.pass_on()
    u_b.begin_z()
    for t in range(3, nz):
        o_a.along(t)
    q_a.across(2)
    q_a.across(1)
    u_b.along(2)
    shift_columns(outside, late)
    u_a.begin_z()
    o_a.across(2)
    local[6].wait()
    d_a.begin_y()
    for t in range(3, nz):
        q_b.across(t)
    d_b.begin_y()
    u_b.along(1)
    q_b.across(1)
    for t in range(3, nz):
        o_a.across(t)
    for sent in spread:
        for copy in sent:
            copy.wait_recv()
    for t in range(3, nz):
        q_a.across(t)
    for t in range(3, nz):
        u_b.along(t)
    u_a.along(2)
    d_a.begin_z()
    for copy in local[7:]:
        copy.wait()
    q_a.arrive_all()
    q_b.arrive_all()
    o_a.across(1)
    project(0, 0)
    lax.fori_loop(1, bands, project_attend, 0)
    attend(bands - 1, 0)
    u_a.pass_on()
    for t in range(3, nz):
        u_b.across(t)
    for t in range(3, nz):
        u_a.along(t)
    o_a.beyond()
    lax.fori_loop(0, bands, go_home, 0)
    u_a.along(1)
    d_b.begin_z()
    u_a.across(2)
    u_b.across(2)
    d_a.along(2)
    for t in range(3, nz):
        u_a.across(t)
    d_b.along(2)
    u_a.across(1)
    o_a.arrive_all()
    d_a.pass_on()
    d_b.pass_on()
    u_b.across(1)
    lax.fori_loop(0, bands, mix, 0)
    d_a.along(1)
    d_a.across(2)
    d_b.across(2)
    u_a.arrive_all()
    u_b.arrive_all()
    d_b.along(1)
    for r in range(1, n_row):
        raise_slot(r)
    for t in range(3, nz):
        d_a.along(t)
    lower(0)
    lower(2)
    for t in range(3, nz):
        d_b.along(t)
    d_b.across(1)
    d_a.across(1)
    lower(1)
    for t in range(3, nz):
        d_a.across(t)
    for t in range(3, nz):
        d_b.across(t)
    for t in range(3, nz):
        lower(t)
    raise_slot(0)
    lower_own(0)
    lower_own(2)
    for t in [1] + list(range(3, nz)):
        lower_own(t)
    for copy in lowered:
        copy.wait_recv()
    for i in range(steps):
        part = slice(i * chunk, (i + 1) * chunk)
        pieces = []
        for z in range(nz):
            total = down_own[z, part, :]
            for r in range(1, n_row):
                total = total + down_recv[r, z, part, :].astype(F32)
            pieces.append(total)
        base = mixed_all[0, part, :].astype(F32)
        total = to_sphere(jnp.concatenate(pieces, axis=1))
        out[part, :] = to_sphere(base + mlp_rate[...] * (total - base)).astype(BF)
    for copy, when in links.started:
        if when is None:
            copy.wait_send()
        else:
            pl.when(when)(copy.wait_send)

    def drain(b, carry):
        for k in range(1, per_window):
            kv_copy(b, k).wait_send()
        back_copy(b).wait_send()
        for r in range(1, n_row):
            home_copy(b, r).wait_send()
        return carry

    lax.fori_loop(0, bands, drain, 0)


def on_device(
    tokens,
    shifts,
    qkv_weight,
    out_weight,
    up_weight,
    down_weight,
    qk_gain,
    attn_rate,
    mlp_rate,
    hidden_gain,
):
    n_row = lax.axis_size("row")
    n_col = lax.axis_size("col")
    local_rows, cols, depth = tokens.shape
    width = qkv_weight.shape[2]
    hidden = up_weight.shape[1]
    own = local_rows * cols
    rows = local_rows * n_row
    count = rows * cols
    bands = rows // WIN
    per_window = WIN // cols
    share = depth // n_col
    nz = n_col // 4
    span = 4 * share
    steps = own // (WIN * cols)
    copies = 7 * (4 * nz + 2) + steps * n_row + (n_row - 1) * (5 * nz + 1)
    dma = pltpu.SemaphoreType.DMA
    dims = (local_rows, cols, depth, width, hidden)

    def layer(side, *operands):
        return pl.pallas_call(
        functools.partial(layer_kernel, n_row, n_col, dims, side),
        out_shape=jax.ShapeDtypeStruct((own, depth), BF),
        in_specs=[SMEM] + [ANY] * 9,
        out_specs=VMEM,
        scratch_shapes=[
            pltpu.VMEM((depth, 3 * width), BF),
            pltpu.VMEM((n_row, depth, width), BF),
            pltpu.VMEM((depth, hidden), BF),
            pltpu.VMEM((depth, hidden), BF),
            pltpu.VMEM((own, depth), BF),
            pltpu.VMEM((2, own, depth), BF),
            pltpu.VMEM((n_row, own, depth), BF),
            pltpu.VMEM((n_row, own, depth), BF),
            pltpu.VMEM((count, width), BF),
            pltpu.VMEM((per_window, 2, count, width), BF),
            pltpu.VMEM((2, count, width), BF),
            pltpu.VMEM((n_row, count, width), BF),
            pltpu.VMEM((n_row, own, depth), BF),
            pltpu.VMEM((n_row, own, hidden), BF),
            pltpu.VMEM((n_row, nz, own, span), BF),
            pltpu.VMEM((n_row, nz, own, span), BF),
            pltpu.VMEM((nz, own, span), F32),
            dma((11,)),
            dma((copies,)),
            dma((copies,)),
            dma((bands, per_window)),
            dma((bands, per_window)),
            dma((bands,)),
            dma((bands,)),
            dma((bands, n_row)),
            dma((bands, n_row)),
            pltpu.VMEM((1, width), F32),
            pltpu.VMEM((1, depth), F32),
            pltpu.VMEM((1, depth), F32),
            pltpu.VMEM((1, hidden), F32),
        ],
        compiler_params=pltpu.CompilerParams(
            collective_id=0 if side > 0 else 1, has_side_effects=True, vmem_limit_bytes=62 * 1024 * 1024
        ),
        name="layer",
    )(*operands)

    result = lax.cond(
        shifts[1] < cols,
        functools.partial(layer, 1),
        functools.partial(layer, -1),
        shifts,
        tokens.reshape(own, depth),
        qkv_weight.transpose(1, 0, 2),
        out_weight.T,
        up_weight,
        down_weight.T,
        qk_gain.reshape(1, width),
        attn_rate.reshape(1, depth),
        mlp_rate.reshape(1, depth),
        hidden_gain.reshape(1, hidden),
    )
    return result.reshape(local_rows, cols, depth)


def solution(mesh):
    return jax.shard_map(
        on_device,
        mesh=mesh,
        in_specs=(
            P("row", "col", None),
            P(),
            P("col", None, "row"),
            P("row", "col"),
            P("col", "row"),
            P("row", "col"),
            P("row"),
            P(),
            P(),
            P("row"),
        ),
        out_specs=P("row", "col", None),
        check_vma=False,
    )
```

```python
import functools
import math

import jax
import jax.numpy as jnp
from jax import lax
from jax.experimental import pallas as pl
from jax.experimental.pallas import tpu as pltpu
from jax.sharding import PartitionSpec as P

HD = 64
WIN = 16
LANES = 128
EPS = 1e-06
BF = jnp.bfloat16
F32 = jnp.float32
MESH = pl.DeviceIdType.MESH
VMEM = pl.BlockSpec(memory_space=pltpu.VMEM)
HBM = pl.BlockSpec(memory_space=pltpu.HBM)
SMEM = pl.BlockSpec(memory_space=pltpu.SMEM)
LAST = (((1,), (1,)), ((), ()))


def to_sphere(vector):
    return vector * lax.rsqrt(jnp.mean(vector * vector, axis=-1, keepdims=True) + EPS)


class Links:
    def __init__(self, n_row, n_col, side, send_sem, recv_sem):
        self.side = side
        self.n_row, self.n_col, self.nz = n_row, n_col, n_col // 4
        self.send_sem, self.recv_sem = send_sem, recv_sem
        self.row, self.col = lax.axis_index("row"), lax.axis_index("col")
        self.z, self.y, self.core = self.col // 4, (self.col // 2) % 2, self.col % 2
        self.y_peer = (self.row, self.at(self.z, 1 - self.y, self.core))
        self.core_peer = (self.row, self.at(self.z, self.y, 1 - self.core))
        self.after = (self.row, lax.rem(self.col + 1, n_col))
        self.before = (self.row, lax.rem(self.col + n_col - 1, n_col))
        self.started = []

    def at(self, z, y, core):
        return (lax.rem(z + 2 * self.nz, self.nz) * 2 + y) * 2 + core

    def along(self, t):
        return (self.row, self.at(self.z + t, self.y, self.core))

    def turn(self, t):
        return t if self.side > 0 else (self.nz - t) % self.nz

    def other_row(self, r):
        return (lax.rem(self.row + r, self.n_row), self.col)

    def greet(self, more):
        peers = [self.y_peer, self.core_peer, self.after, self.before]
        peers += [self.along(t) for t in range(1, self.nz)]
        peers += more + [self.other_row(r) for r in range(1, self.n_row)]
        barrier = pltpu.get_barrier_semaphore()
        for peer in peers:
            pl.semaphore_signal(barrier, inc=1, device_id=peer, device_id_type=MESH)
        pl.semaphore_wait(barrier, len(peers))

    def make(self, src, dst, peer, when=None, landing=None):
        index = len(self.started)
        copy = pltpu.make_async_remote_copy(
            src_ref=src,
            dst_ref=dst,
            send_sem=self.send_sem.at[index],
            recv_sem=self.recv_sem.at[index if landing is None else landing],
            device_id=peer,
            device_id_type=MESH,
        )
        self.started.append((copy, when))
        return copy

    def send(self, src, dst, peer, when=None, landing=None):
        copy = self.make(src, dst, peer, when, landing)
        if when is None:
            copy.start()
        else:
            pl.when(when)(copy.start)
        return copy


class Spread:
    def __init__(self, links, full, depth, low, size, relief, relay, rows=()):
        self.links, self.full, self.depth, self.low, self.size = links, full, depth, low, size
        self.relief = relief and links.nz > 1
        self.relay = relay and links.nz > 2
        self.rows = rows
        self.z_copy, self.y_copy, self.core_copy, self.row_copy = {}, {}, {}, {}
        self.z_index, self.y_index = {}, {}
        for t in range(links.nz):
            when = None
            if self.relief and t in (1, links.nz - 1):
                when = links.z % 2 == (0 if t == 1 else 1)
            block = self.block(links.z - t, links.y)
            self.y_index[t] = len(links.started)
            self.y_copy[t] = links.make(block, block, links.y_peer, when)

    def place(self, z, y):
        owner = self.links.at(z, y, self.links.core)
        return pl.ds(pl.multiple_of(owner * self.depth + self.low, self.size), self.size)

    def block(self, z, y):
        return self.full.at[self.place(z, y)]

    def to_core(self, name, block):
        links = self.links
        self.core_copy[name] = links.send(block, block, links.core_peer)
        for r, there in self.rows:
            z = links.z - name[1]
            place = self.place(z, links.y if name[0] == "z" else 1 - links.y)
            self.row_copy[name, r] = links.send(block, there.at[place], links.other_row(r))

    def beyond(self):
        links = self.links
        for t in range(links.nz):
            for kind, y in (("z", links.y), ("y", 1 - links.y)):
                for r, there in self.rows:
                    self.row_copy[(kind, t), r].wait_recv()
                    block = there.at[self.place(links.z - t, y)]
                    self.core_copy[kind, t, r] = links.send(block, block, links.core_peer)

    def begin_z(self):
        links = self.links
        nz = links.nz
        own = self.block(links.z, links.y)
        for t in map(links.turn, sorted(range(1, nz), key=lambda t: -min(t, nz - t))):
            when = None
            if self.relay:
                when = {1: links.z != nz - 1, nz - 1: links.z != 0}.get(t)
            self.z_index[t] = len(links.started)
            self.z_copy[t] = links.send(own, own, links.along(t), when)
        self.to_core(("z", 0), own)

    def to_y(self, t):
        when = self.links.started[self.y_index[t]][1]
        if when is None:
            self.y_copy[t].start()
        else:
            pl.when(when)(self.y_copy[t].start)

    def begin_y(self):
        self.to_y(0)

    def begin(self):
        self.begin_z()
        self.begin_y()

    def along(self, t):
        links = self.links
        t = links.turn(t)
        nz = links.nz
        self.z_copy[t].wait_recv()
        block = self.block(links.z - t, links.y)
        if self.relay and t == 2:
            links.send(block, block, links.along(nz - 1), links.z == 1, self.z_index[1])
        if self.relay and t == nz - 2:
            links.send(block, block, links.along(1), links.z == nz - 2, self.z_index[nz - 1])
        self.to_y(t)
        self.to_core(("z", t), block)

    def across(self, t):
        t = self.links.turn(t)
        self.y_copy[t].wait_recv()
        self.to_core(("y", t), self.block(self.links.z - t, 1 - self.links.y))

    def pass_on(self):
        links = self.links
        self.across(0)
        if self.relief:
            block = self.block(links.z, 1 - links.y)
            even = links.z % 2 == 0
            partner = (links.row, links.at(links.z + 1 - 2 * (links.z % 2), links.y, links.core))
            landing = jnp.where(even, self.y_index[1], self.y_index[links.nz - 1])
            links.send(block, block, partner, None, landing)

    def arrive(self, t):
        t = self.links.turn(t)
        self.core_copy["z", t].wait_recv()
        self.core_copy["y", t].wait_recv()

    def arrive_all(self):
        for copy in self.core_copy.values():
            copy.wait_recv()


def layer_kernel(n_row, n_col, dims, side, *refs):
    local_rows, cols, depth, width, hidden = dims
    shifts, tok_in, q_in, o_in, u_in, d_in = refs[:6]
    vectors, out = refs[6:10], refs[10]
    q_full, o_all, u_full, d_full, tok, piece, sphere_all = refs[11:18]
    strip, q_all, kv_all, back, home_all = refs[18:23]
    mixed_all, active, down_send, down_recv, down_own = refs[23:28]
    local_sem, send_sem, recv_sem, kv_send, kv_recv, back_send, back_recv = refs[28:35]
    home_send, home_recv, gain, attn_rate, mlp_rate, hidden_gain = refs[35:]

    links = Links(n_row, n_col, side, send_sem, recv_sem)
    row, col, nz = links.row, links.col, links.nz
    own = local_rows * cols
    rows = local_rows * n_row
    band = WIN * cols
    bands = rows // WIN
    per_window = WIN // cols
    share = depth // n_col
    seat = lax.rem(col, per_window)
    shift_row, shift_col = shifts[0], shifts[1]
    mine = 0 if side > 0 else 1
    first = shift_col if side > 0 else shift_col - cols

    def mate(k):
        return (row, col - seat + lax.rem(seat + k, per_window))

    here = pl.ds(pl.multiple_of(col * share, share), share)
    local = [
        pltpu.make_async_copy(src, dst, local_sem.at[i])
        for i, (src, dst) in enumerate(
            [(q_in.at[p], q_full.at[here, pl.ds(p * width, width)]) for p in range(3)]
            + [
                (tok_in, tok),
                (o_in, o_all.at[0, here]),
                (u_in, u_full.at[here]),
                (d_in, d_full.at[here]),
            ]
            + list(zip(vectors, (gain, attn_rate, mlp_rate, hidden_gain)))
        )
    ]
    for copy in local:
        copy.start()
    source, target = (links.after, links.before) if side > 0 else (links.before, links.after)
    links.greet([mate(k) for k in range(1, per_window)])

    half = share // 2
    q_a = Spread(links, q_full, share, 0, half, True, False)
    q_b = Spread(links, q_full, share, half, half, False, True)
    o_rows = [(r, o_all.at[r]) for r in range(1, n_row)]
    o_a = Spread(links, o_all.at[0], share, 0, share, False, True, o_rows)
    u_a = Spread(links, u_full, share, 0, half, True, True)
    u_b = Spread(links, u_full, share, half, half, False, True)
    d_a = Spread(links, d_full, share, 0, half, False, True)
    d_b = Spread(links, d_full, share, half, half, True, True)

    chunk = band
    steps = own // chunk
    half_steps = steps // 2
    early, late = range(half_steps), range(half_steps, steps)
    halo = [
        links.make(
            piece.at[mine, pl.ds(i * chunk, chunk)],
            piece.at[1 - mine, pl.ds(i * chunk, chunk)],
            target,
        )
        for i in range(steps)
    ]
    bits = cols.bit_length() - 1

    def one_hot(length, row_step, column_step, per_piece):
        token = lax.broadcasted_iota(jnp.int32, (band, length), 0)
        source = lax.broadcasted_iota(jnp.int32, (band, length), 1)
        which = lax.shift_right_logical(source, per_piece.bit_length() - 1)
        source = source & (per_piece - 1)
        same_row = lax.shift_right_logical(source, bits) == (
            lax.shift_right_logical(token, bits) + row_step
        )
        same_column = which * cols + (source & (cols - 1)) == (token & (cols - 1)) + column_step
        return jnp.where(same_row & same_column, 1.0, 0.0).astype(BF)

    to_columns = one_hot(2 * band, 0, first, band)
    to_rows = one_hot(2 * band, shift_row, 0, 2 * band)
    to_home = one_hot(4 * band, WIN - shift_row, cols - first, 2 * band)

    spread = [
        [
            links.make(
                strip.at[0, pl.ds(i * chunk, chunk)],
                strip.at[r, pl.ds(i * chunk, chunk)],
                links.other_row(r),
            )
            for r in range(1, n_row)
        ]
        for i in range(steps)
    ]

    inside = links.core == (0 if side > 0 else 1)
    outside = jnp.logical_not(inside)

    def shift_columns(who, which):
        @pl.when(who)
        def _():
            for i in which:
                part = slice(i * chunk, (i + 1) * chunk)
                halo[i].wait_recv()
                near = jnp.concatenate([piece[k, part, :] for k in range(2)], axis=0)
                strip[0, part, :] = jnp.dot(
                    to_columns, near, preferred_element_type=F32
                ).astype(BF)
                for copy in spread[i]:
                    copy.start()

    group = (lax.broadcasted_iota(jnp.int32, (LANES, LANES), 0) < HD) == (
        lax.broadcasted_iota(jnp.int32, (LANES, LANES), 1) < HD
    )
    averaging = jnp.where(group, 1.0 / HD, 0.0).astype(BF)

    def band_rows(b):
        return pl.ds(pl.multiple_of(b * band, band), band)

    def kv_copy(b, k):
        return pltpu.make_async_remote_copy(
            src_ref=kv_all.at[0, :, band_rows(b)],
            dst_ref=kv_all.at[k, :, band_rows(b)],
            send_sem=kv_send.at[b, k],
            recv_sem=kv_recv.at[b, k],
            device_id=mate(k),
            device_id_type=MESH,
        )

    def back_copy(b):
        return pltpu.make_async_remote_copy(
            src_ref=back.at[1 - mine, band_rows(b)],
            dst_ref=back.at[mine, band_rows(b)],
            send_sem=back_send.at[b],
            recv_sem=back_recv.at[b],
            device_id=source,
            device_id_type=MESH,
        )

    def home_copy(b, r):
        return pltpu.make_async_remote_copy(
            src_ref=home_all.at[0, band_rows(b)],
            dst_ref=home_all.at[r, band_rows(b)],
            send_sem=home_send.at[b, r],
            recv_sem=home_recv.at[b, r],
            device_id=links.other_row(r),
            device_id_type=MESH,
        )

    def block_of(b):
        slot = lax.rem(row - b // steps + n_row, n_row)
        return strip[slot, pl.ds(pl.multiple_of(lax.rem(b, steps) * band, band), band), :]

    def project(b, carry):
        near = jnp.concatenate([block_of(b), block_of(lax.rem(b + 1, bands))], axis=0)
        x = jnp.dot(to_rows, near, preferred_element_type=F32).astype(BF)
        for part in range(3):
            got = jnp.dot(
                x, q_full[:, part * width : (part + 1) * width], preferred_element_type=F32
            )
            if part == 2:
                kv_all[0, 1, band_rows(b), :] = got.astype(BF)
                continue
            for lo in range(0, width, LANES):
                cut = slice(lo, lo + LANES)
                one = got[:, cut]
                mean = jnp.dot((one * one).astype(BF), averaging, preferred_element_type=F32)
                scaled = one * lax.rsqrt(mean + EPS) * gain[:, cut]
                if part == 0:
                    q_all[band_rows(b), cut] = (scaled * (1.0 / math.sqrt(HD))).astype(BF)
                else:
                    kv_all[0, 0, band_rows(b), cut] = scaled.astype(BF)
        for k in range(1, per_window):
            kv_copy(b, k).start()
        return carry

    lane = lax.broadcasted_iota(jnp.int32, (band, LANES), 1) < HD

    def attend(b, carry):
        for k in range(1, per_window):
            kv_copy(b, k).wait_recv()
        for lo in range(0, width, LANES):
            cut = slice(lo, lo + LANES)
            query = q_all[band_rows(b), cut].astype(F32)
            both = jnp.concatenate(
                [jnp.where(lane, query, 0.0), jnp.where(lane, 0.0, query)], axis=0
            ).astype(BF)
            keys = jnp.concatenate(
                [kv_all[k, 0, band_rows(b), cut] for k in range(per_window)], axis=0
            )
            values = jnp.concatenate(
                [kv_all[k, 1, band_rows(b), cut] for k in range(per_window)], axis=0
            )
            scores = lax.dot_general(both, keys, LAST, preferred_element_type=F32)
            expo = jnp.exp(scores)
            total = jnp.sum(expo, axis=-1, keepdims=True)
            got = jnp.dot(expo.astype(BF), values, preferred_element_type=F32) / total
            got = jnp.where(lane, got[:band], got[band:]).astype(BF)
            back[1 - mine, band_rows(b), cut] = got
        back_copy(b).start()
        return carry

    def project_attend(b, carry):
        project(b, 0)
        attend(b - 1, 0)
        return carry

    def go_home(j, carry):
        b = lax.rem(j + 1, bands)

        @pl.when(j == 0)
        def _():
            back_copy(0).wait_recv()

        @pl.when(j < bands - 1)
        def _():
            back_copy(b).wait_recv()

        earlier = lax.rem(b + bands - 1, bands)
        near = jnp.concatenate(
            [back[k, band_rows(at), :] for k in range(2) for at in (earlier, b)], axis=0
        )
        home_all[0, band_rows(b), :] = jnp.dot(
            to_home, near, preferred_element_type=F32
        ).astype(BF)
        for r in range(1, n_row):
            home_copy(b, r).start()
        return carry

    def mix(j, carry):
        b = lax.rem(j + 1, bands)
        slot = lax.rem(row - b // steps + n_row, n_row)
        part = pl.ds(pl.multiple_of(lax.rem(b, steps) * chunk, chunk), chunk)
        total = None
        for r in range(n_row):
            if r > 0:
                home_copy(b, r).wait_recv()
            term = lax.dot_general(
                home_all[r, band_rows(b), :], o_all[r], LAST, preferred_element_type=F32
            )
            total = term if total is None else total + term
        base = sphere_all[slot, part, :].astype(F32)
        value = to_sphere(base + attn_rate[...] * (to_sphere(total) - base))
        mixed_all[slot, part, :] = value.astype(BF)
        return carry

    tile = min(512, hidden)

    def raise_slot(r):
        def raise_tile(i, carry):
            cut = pl.ds(pl.multiple_of(i * tile, tile), tile)
            raised = jnp.dot(mixed_all[r], u_full[:, cut], preferred_element_type=F32)
            raised = raised * hidden_gain[:, cut]
            active[r, :, cut] = (
                0.5 * raised * (1.0 + lax.erf(raised * (1.0 / math.sqrt(2.0))))
            ).astype(BF)
            return carry

        lax.fori_loop(0, hidden // tile, raise_tile, 0)

    span = 4 * share
    lowered = []

    def lower_to(r, t):
        z = lax.rem(links.z - links.turn(t) + nz, nz)
        weight = d_full[pl.ds(pl.multiple_of(z * span, span), span), :]
        return z, lax.dot_general(active[r], weight, LAST, preferred_element_type=F32)

    def lower(t):
        d_a.arrive(t)
        d_b.arrive(t)
        for r in range(1, n_row):
            z, got = lower_to(r, t)
            down_send[r, z] = got.astype(BF)
            lowered.append(
                links.send(
                    down_send.at[r, z], down_recv.at[r, z], links.other_row(n_row - r)
                )
            )

    def lower_own(t):
        z, got = lower_to(0, t)
        down_own[z] = got

    def to_neighbour():
        for i in range(steps):
            part = slice(i * chunk, (i + 1) * chunk)
            value = to_sphere(tok[part, :].astype(F32)).astype(BF)
            sphere_all[0, part, :] = value
            piece[mine, part, :] = value

    for copy in local[:3]:
        copy.wait()
    q_b.begin_z()
    q_b.begin_y()
    local[5].wait()
    u_b.begin_y()
    local[4].wait()
    o_a.begin_y()
    local[3].wait()
    to_neighbour()
    for i in early:
        halo[i].start()
    around = [
        links.send(sphere_all.at[0], sphere_all.at[r], links.other_row(r))
        for r in range(1, n_row)
    ]
    shift_columns(inside, early)
    q_a.begin_z()
    q_a.begin_y()
    for i in late:
        halo[i].start()
    q_b.along(2)
    for copy in around:
        copy.wait_recv()
    o_a.begin_z()
    q_b.along(1)
    u_a.begin_y()
    shift_columns(outside, early)
    u_b.pass_on()
    q_b.pass_on()
    q_b.across(2)
    shift_columns(inside, late)
    q_a.pass_on()
    q_a.along(2)
    q_a.along(1)
    for t in range(3, nz):
        q_b.along(t)
    for t in range(3, nz):
        q_a.along(t)
    o_a.along(2)
    o_a.along(1)
    o_a.pass_on()
    u_b.begin_z()
    for t in range(3, nz):
        o_a.along(t)
    q_a.across(2)
    q_a.across(1)
    u_b.along(2)
    shift_columns(outside, late)
    u_a.begin_z()
    o_a.across(2)
    local[6].wait()
    d_a.begin_y()
    for t in range(3, nz):
        q_b.across(t)
    d_b.begin_y()
    u_b.along(1)
    q_b.across(1)
    for t in range(3, nz):
        o_a.across(t)
    for sent in spread:
        for copy in sent:
            copy.wait_recv()
    for t in range(3, nz):
        q_a.across(t)
    for t in range(3, nz):
        u_b.along(t)
    u_a.along(2)
    d_a.begin_z()
    for copy in local[7:]:
        copy.wait()
    q_a.arrive_all()
    q_b.arrive_all()
    o_a.across(1)
    project(0, 0)
    lax.fori_loop(1, bands, project_attend, 0)
    attend(bands - 1, 0)
    u_a.pass_on()
    for t in range(3, nz):
        u_b.across(t)
    for t in range(3, nz):
        u_a.along(t)
    o_a.beyond()
    lax.fori_loop(0, bands, go_home, 0)
    u_a.along(1)
    d_b.begin_z()
    u_a.across(2)
    u_b.across(2)
    d_a.along(2)
    for t in range(3, nz):
        u_a.across(t)
    d_b.along(2)
    u_a.across(1)
    o_a.arrive_all()
    d_a.pass_on()
    d_b.pass_on()
    u_b.across(1)
    lax.fori_loop(0, bands, mix, 0)
    d_a.along(1)
    d_a.across(2)
    d_b.across(2)
    u_a.arrive_all()
    u_b.arrive_all()
    d_b.along(1)
    for r in range(1, n_row):
        raise_slot(r)
    for t in range(3, nz):
        d_a.along(t)
    lower(0)
    lower(2)
    for t in range(3, nz):
        d_b.along(t)
    d_b.across(1)
    d_a.across(1)
    lower(1)
    for t in range(3, nz):
        d_a.across(t)
    for t in range(3, nz):
        d_b.across(t)
    for t in range(3, nz):
        lower(t)
    raise_slot(0)
    lower_own(0)
    lower_own(2)
    for t in [1] + list(range(3, nz)):
        lower_own(t)
    for copy in lowered:
        copy.wait_recv()
    for i in range(steps):
        part = slice(i * chunk, (i + 1) * chunk)
        pieces = []
        for z in range(nz):
            total = down_own[z, part, :]
            for r in range(1, n_row):
                total = total + down_recv[r, z, part, :].astype(F32)
            pieces.append(total)
        base = mixed_all[0, part, :].astype(F32)
        total = to_sphere(jnp.concatenate(pieces, axis=1))
        out[part, :] = to_sphere(base + mlp_rate[...] * (total - base)).astype(BF)
    for copy, when in links.started:
        if when is None:
            copy.wait_send()
        else:
            pl.when(when)(copy.wait_send)

    def drain(b, carry):
        for k in range(1, per_window):
            kv_copy(b, k).wait_send()
        back_copy(b).wait_send()
        for r in range(1, n_row):
            home_copy(b, r).wait_send()
        return carry

    lax.fori_loop(0, bands, drain, 0)


def on_device(
    tokens,
    shifts,
    qkv_weight,
    out_weight,
    up_weight,
    down_weight,
    qk_gain,
    attn_rate,
    mlp_rate,
    hidden_gain,
):
    n_row = lax.axis_size("row")
    n_col = lax.axis_size("col")
    local_rows, cols, depth = tokens.shape
    width = qkv_weight.shape[2]
    hidden = up_weight.shape[1]
    own = local_rows * cols
    rows = local_rows * n_row
    count = rows * cols
    bands = rows // WIN
    per_window = WIN // cols
    share = depth // n_col
    nz = n_col // 4
    span = 4 * share
    steps = own // (WIN * cols)
    copies = 7 * (4 * nz + 2) + steps * n_row + (n_row - 1) * (5 * nz + 1)
    dma = pltpu.SemaphoreType.DMA
    dims = (local_rows, cols, depth, width, hidden)
    room = 67043328 - own * depth * 2 - 2048

    def layer(side, *operands):
        return pl.pallas_call(
        functools.partial(layer_kernel, n_row, n_col, dims, side),
        out_shape=jax.ShapeDtypeStruct((own, depth), BF),
        in_specs=[SMEM] + [HBM] * 9,
        out_specs=VMEM,
        scratch_shapes=[
            pltpu.VMEM((depth, 3 * width), BF),
            pltpu.VMEM((n_row, depth, width), BF),
            pltpu.VMEM((depth, hidden), BF),
            pltpu.VMEM((depth, hidden), BF),
            pltpu.VMEM((own, depth), BF),
            pltpu.VMEM((2, own, depth), BF),
            pltpu.VMEM((n_row, own, depth), BF),
            pltpu.VMEM((n_row, own, depth), BF),
            pltpu.VMEM((count, width), BF),
            pltpu.VMEM((per_window, 2, count, width), BF),
            pltpu.VMEM((2, count, width), BF),
            pltpu.VMEM((n_row, count, width), BF),
            pltpu.VMEM((n_row, own, depth), BF),
            pltpu.VMEM((n_row, own, hidden), BF),
            pltpu.VMEM((n_row, nz, own, span), BF),
            pltpu.VMEM((n_row, nz, own, span), BF),
            pltpu.VMEM((nz, own, span), F32),
            dma((11,)),
            dma((copies,)),
            dma((copies,)),
            dma((bands, per_window)),
            dma((bands, per_window)),
            dma((bands,)),
            dma((bands,)),
            dma((bands, n_row)),
            dma((bands, n_row)),
            pltpu.VMEM((1, width), F32),
            pltpu.VMEM((1, depth), F32),
            pltpu.VMEM((1, depth), F32),
            pltpu.VMEM((1, hidden), F32),
        ],
        compiler_params=pltpu.CompilerParams(
            collective_id=0 if side > 0 else 1, has_side_effects=True, vmem_limit_bytes=room
        ),
        name="layer",
    )(*operands)

    result = lax.cond(
        shifts[1] < cols,
        functools.partial(layer, 1),
        functools.partial(layer, -1),
        shifts,
        tokens.reshape(own, depth),
        qkv_weight.transpose(1, 0, 2),
        out_weight.T,
        up_weight,
        down_weight.T,
        qk_gain.reshape(1, width),
        attn_rate.reshape(1, depth),
        mlp_rate.reshape(1, depth),
        hidden_gain.reshape(1, hidden),
    )
    return result.reshape(local_rows, cols, depth)


def solution(mesh):
    return jax.shard_map(
        on_device,
        mesh=mesh,
        in_specs=(
            P("row", "col", None),
            P(),
            P("col", None, "row"),
            P("row", "col"),
            P("col", "row"),
            P("row", "col"),
            P("row"),
            P(),
            P(),
            P("row"),
        ),
        out_specs=P("row", "col", None),
        check_vma=False,
    )
```

```python
import functools
import math

import jax
import jax.numpy as jnp
from jax import lax
from jax.experimental import pallas as pl
from jax.experimental.pallas import tpu as pltpu
from jax.sharding import PartitionSpec as P

HD = 64
WIN = 16
LANES = 128
EPS = 1e-06
BF = jnp.bfloat16
F32 = jnp.float32
MESH = pl.DeviceIdType.MESH
VMEM = pl.BlockSpec(memory_space=pltpu.VMEM)
HBM = pl.BlockSpec(memory_space=pltpu.HBM)
SMEM = pl.BlockSpec(memory_space=pltpu.SMEM)
LAST = (((1,), (1,)), ((), ()))


def to_sphere(vector):
    return vector * lax.rsqrt(jnp.mean(vector * vector, axis=-1, keepdims=True) + EPS)


class Links:
    def __init__(self, n_row, n_col, side, send_sem, recv_sem):
        self.side = side
        self.n_row, self.n_col, self.nz = n_row, n_col, n_col // 4
        self.send_sem, self.recv_sem = send_sem, recv_sem
        self.row, self.col = lax.axis_index("row"), lax.axis_index("col")
        self.z, self.y, self.core = self.col // 4, (self.col // 2) % 2, self.col % 2
        self.y_peer = (self.row, self.at(self.z, 1 - self.y, self.core))
        self.core_peer = (self.row, self.at(self.z, self.y, 1 - self.core))
        self.after = (self.row, lax.rem(self.col + 1, n_col))
        self.before = (self.row, lax.rem(self.col + n_col - 1, n_col))
        self.started = []

    def at(self, z, y, core):
        return (lax.rem(z + 2 * self.nz, self.nz) * 2 + y) * 2 + core

    def along(self, t):
        return (self.row, self.at(self.z + t, self.y, self.core))

    def turn(self, t):
        return t if self.side > 0 else (self.nz - t) % self.nz

    def other_row(self, r):
        return (lax.rem(self.row + r, self.n_row), self.col)

    def greet(self, more):
        peers = [self.y_peer, self.core_peer, self.after, self.before]
        peers += [self.along(t) for t in range(1, self.nz)]
        peers += more + [self.other_row(r) for r in range(1, self.n_row)]
        barrier = pltpu.get_barrier_semaphore()
        for peer in peers:
            pl.semaphore_signal(barrier, inc=1, device_id=peer, device_id_type=MESH)
        pl.semaphore_wait(barrier, len(peers))

    def make(self, src, dst, peer, when=None, landing=None):
        index = len(self.started)
        copy = pltpu.make_async_remote_copy(
            src_ref=src,
            dst_ref=dst,
            send_sem=self.send_sem.at[index],
            recv_sem=self.recv_sem.at[index if landing is None else landing],
            device_id=peer,
            device_id_type=MESH,
        )
        self.started.append((copy, when))
        return copy

    def send(self, src, dst, peer, when=None, landing=None):
        copy = self.make(src, dst, peer, when, landing)
        if when is None:
            copy.start()
        else:
            pl.when(when)(copy.start)
        return copy


class Spread:
    def __init__(self, links, full, depth, low, size, relief, relay, rows=()):
        self.links, self.full, self.depth, self.low, self.size = links, full, depth, low, size
        self.relief = relief and links.nz > 1
        self.relay = relay and links.nz > 2
        self.rows = rows
        self.z_copy, self.y_copy, self.core_copy, self.row_copy = {}, {}, {}, {}
        self.z_index, self.y_index = {}, {}
        for t in range(links.nz):
            when = None
            if self.relief and t in (1, links.nz - 1):
                when = links.z % 2 == (0 if t == 1 else 1)
            block = self.block(links.z - t, links.y)
            self.y_index[t] = len(links.started)
            self.y_copy[t] = links.make(block, block, links.y_peer, when)

    def place(self, z, y):
        owner = self.links.at(z, y, self.links.core)
        return pl.ds(pl.multiple_of(owner * self.depth + self.low, self.size), self.size)

    def block(self, z, y):
        return self.full.at[self.place(z, y)]

    def to_core(self, name, block):
        links = self.links
        self.core_copy[name] = links.send(block, block, links.core_peer)
        for r, there in self.rows:
            z = links.z - name[1]
            place = self.place(z, links.y if name[0] == "z" else 1 - links.y)
            self.row_copy[name, r] = links.send(block, there.at[place], links.other_row(r))

    def beyond(self):
        links = self.links
        for t in range(links.nz):
            for kind, y in (("z", links.y), ("y", 1 - links.y)):
                for r, there in self.rows:
                    self.row_copy[(kind, t), r].wait_recv()
                    block = there.at[self.place(links.z - t, y)]
                    self.core_copy[kind, t, r] = links.send(block, block, links.core_peer)

    def begin_z(self):
        links = self.links
        nz = links.nz
        own = self.block(links.z, links.y)
        for t in map(links.turn, sorted(range(1, nz), key=lambda t: -min(t, nz - t))):
            when = None
            if self.relay:
                when = {1: links.z != nz - 1, nz - 1: links.z != 0}.get(t)
            self.z_index[t] = len(links.started)
            self.z_copy[t] = links.send(own, own, links.along(t), when)
        self.to_core(("z", 0), own)

    def to_y(self, t):
        when = self.links.started[self.y_index[t]][1]
        if when is None:
            self.y_copy[t].start()
        else:
            pl.when(when)(self.y_copy[t].start)

    def begin_y(self):
        self.to_y(0)

    def begin(self):
        self.begin_z()
        self.begin_y()

    def along(self, t):
        links = self.links
        t = links.turn(t)
        nz = links.nz
        self.z_copy[t].wait_recv()
        block = self.block(links.z - t, links.y)
        if self.relay and t == 2:
            links.send(block, block, links.along(nz - 1), links.z == 1, self.z_index[1])
        if self.relay and t == nz - 2:
            links.send(block, block, links.along(1), links.z == nz - 2, self.z_index[nz - 1])
        self.to_y(t)
        self.to_core(("z", t), block)

    def across(self, t):
        t = self.links.turn(t)
        self.y_copy[t].wait_recv()
        self.to_core(("y", t), self.block(self.links.z - t, 1 - self.links.y))

    def pass_on(self):
        links = self.links
        self.across(0)
        if self.relief:
            block = self.block(links.z, 1 - links.y)
            even = links.z % 2 == 0
            partner = (links.row, links.at(links.z + 1 - 2 * (links.z % 2), links.y, links.core))
            landing = jnp.where(even, self.y_index[1], self.y_index[links.nz - 1])
            links.send(block, block, partner, None, landing)

    def arrive(self, t):
        t = self.links.turn(t)
        self.core_copy["z", t].wait_recv()
        self.core_copy["y", t].wait_recv()

    def arrive_all(self):
        for copy in self.core_copy.values():
            copy.wait_recv()


def layer_kernel(n_row, n_col, dims, side, *refs):
    local_rows, cols, depth, width, hidden = dims
    shifts, tok_in, q_in, o_in, u_in, d_in = refs[:6]
    vectors, out = refs[6:10], refs[10]
    q_full, o_all, u_full, d_full, tok, piece, sphere_all = refs[11:18]
    strip, q_all, kv_all, back, home_all = refs[18:23]
    mixed_all, active, down_send, down_recv, down_own = refs[23:28]
    local_sem, send_sem, recv_sem, kv_send, kv_recv, back_send, back_recv = refs[28:35]
    home_send, home_recv, gain, attn_rate, mlp_rate, hidden_gain = refs[35:]

    links = Links(n_row, n_col, side, send_sem, recv_sem)
    row, col, nz = links.row, links.col, links.nz
    own = local_rows * cols
    rows = local_rows * n_row
    band = WIN * cols
    bands = rows // WIN
    per_window = WIN // cols
    share = depth // n_col
    seat = lax.rem(col, per_window)
    shift_row, shift_col = shifts[0], shifts[1]
    mine = 0 if side > 0 else 1
    first = shift_col if side > 0 else shift_col - cols

    def mate(k):
        return (row, col - seat + lax.rem(seat + k, per_window))

    here = pl.ds(pl.multiple_of(col * share, share), share)
    local = [
        pltpu.make_async_copy(src, dst, local_sem.at[i])
        for i, (src, dst) in enumerate(
            [(q_in.at[p], q_full.at[here, pl.ds(p * width, width)]) for p in range(3)]
            + [
                (tok_in, tok),
                (o_in, o_all.at[0, here]),
                (u_in, u_full.at[here]),
                (d_in, d_full.at[here]),
            ]
            + list(zip(vectors, (gain, attn_rate, mlp_rate, hidden_gain)))
        )
    ]
    for copy in local:
        copy.start()
    source, target = (links.after, links.before) if side > 0 else (links.before, links.after)
    links.greet([mate(k) for k in range(1, per_window)])

    half = share // 2
    q_a = Spread(links, q_full, share, 0, half, False, True)
    q_b = Spread(links, q_full, share, half, half, False, True)
    o_rows = [(r, o_all.at[r]) for r in range(1, n_row)]
    o_a = Spread(links, o_all.at[0], share, 0, share, False, True, o_rows)
    u_a = Spread(links, u_full, share, 0, half, True, True)
    u_b = Spread(links, u_full, share, half, half, False, True)
    d_a = Spread(links, d_full, share, 0, half, True, True)
    d_b = Spread(links, d_full, share, half, half, True, True)

    chunk = band
    steps = own // chunk
    half_steps = steps // 2
    early, late = range(half_steps), range(half_steps, steps)
    halo = [
        links.make(
            piece.at[mine, pl.ds(i * chunk, chunk)],
            piece.at[1 - mine, pl.ds(i * chunk, chunk)],
            target,
        )
        for i in range(steps)
    ]
    bits = cols.bit_length() - 1

    def one_hot(length, row_step, column_step, per_piece):
        token = lax.broadcasted_iota(jnp.int32, (band, length), 0)
        source = lax.broadcasted_iota(jnp.int32, (band, length), 1)
        which = lax.shift_right_logical(source, per_piece.bit_length() - 1)
        source = source & (per_piece - 1)
        same_row = lax.shift_right_logical(source, bits) == (
            lax.shift_right_logical(token, bits) + row_step
        )
        same_column = which * cols + (source & (cols - 1)) == (token & (cols - 1)) + column_step
        return jnp.where(same_row & same_column, 1.0, 0.0).astype(BF)

    to_columns = one_hot(2 * band, 0, first, band)
    to_rows = one_hot(2 * band, shift_row, 0, 2 * band)
    to_home = one_hot(4 * band, WIN - shift_row, cols - first, 2 * band)

    spread = [
        [
            links.make(
                strip.at[0, pl.ds(i * chunk, chunk)],
                strip.at[r, pl.ds(i * chunk, chunk)],
                links.other_row(r),
            )
            for r in range(1, n_row)
        ]
        for i in range(steps)
    ]

    inside = links.core == (0 if side > 0 else 1)
    outside = jnp.logical_not(inside)

    def shift_columns(who, which):
        @pl.when(who)
        def _():
            for i in which:
                part = slice(i * chunk, (i + 1) * chunk)
                halo[i].wait_recv()
                near = jnp.concatenate([piece[k, part, :] for k in range(2)], axis=0)
                strip[0, part, :] = jnp.dot(
                    to_columns, near, preferred_element_type=F32
                ).astype(BF)
                for copy in spread[i]:
                    copy.start()

    group = (lax.broadcasted_iota(jnp.int32, (LANES, LANES), 0) < HD) == (
        lax.broadcasted_iota(jnp.int32, (LANES, LANES), 1) < HD
    )
    averaging = jnp.where(group, 1.0 / HD, 0.0).astype(BF)

    def band_rows(b):
        return pl.ds(pl.multiple_of(b * band, band), band)

    def kv_copy(b, k):
        return pltpu.make_async_remote_copy(
            src_ref=kv_all.at[0, :, band_rows(b)],
            dst_ref=kv_all.at[k, :, band_rows(b)],
            send_sem=kv_send.at[b, k],
            recv_sem=kv_recv.at[b, k],
            device_id=mate(k),
            device_id_type=MESH,
        )

    def back_copy(b):
        return pltpu.make_async_remote_copy(
            src_ref=back.at[1 - mine, band_rows(b)],
            dst_ref=back.at[mine, band_rows(b)],
            send_sem=back_send.at[b],
            recv_sem=back_recv.at[b],
            device_id=source,
            device_id_type=MESH,
        )

    def home_copy(b, r):
        return pltpu.make_async_remote_copy(
            src_ref=home_all.at[0, band_rows(b)],
            dst_ref=home_all.at[r, band_rows(b)],
            send_sem=home_send.at[b, r],
            recv_sem=home_recv.at[b, r],
            device_id=links.other_row(r),
            device_id_type=MESH,
        )

    def block_of(b):
        slot = lax.rem(row - b // steps + n_row, n_row)
        return strip[slot, pl.ds(pl.multiple_of(lax.rem(b, steps) * band, band), band), :]

    def project(b, carry):
        near = jnp.concatenate([block_of(b), block_of(lax.rem(b + 1, bands))], axis=0)
        x = jnp.dot(to_rows, near, preferred_element_type=F32).astype(BF)
        for part in range(3):
            got = jnp.dot(
                x, q_full[:, part * width : (part + 1) * width], preferred_element_type=F32
            )
            if part == 2:
                kv_all[0, 1, band_rows(b), :] = got.astype(BF)
                continue
            for lo in range(0, width, LANES):
                cut = slice(lo, lo + LANES)
                one = got[:, cut]
                mean = jnp.dot((one * one).astype(BF), averaging, preferred_element_type=F32)
                scaled = one * lax.rsqrt(mean + EPS) * gain[:, cut]
                if part == 0:
                    q_all[band_rows(b), cut] = (scaled * (1.0 / math.sqrt(HD))).astype(BF)
                else:
                    kv_all[0, 0, band_rows(b), cut] = scaled.astype(BF)
        for k in range(1, per_window):
            kv_copy(b, k).start()
        return carry

    lane = lax.broadcasted_iota(jnp.int32, (band, LANES), 1) < HD

    def attend(b, carry):
        for k in range(1, per_window):
            kv_copy(b, k).wait_recv()
        for lo in range(0, width, LANES):
            cut = slice(lo, lo + LANES)
            query = q_all[band_rows(b), cut].astype(F32)
            both = jnp.concatenate(
                [jnp.where(lane, query, 0.0), jnp.where(lane, 0.0, query)], axis=0
            ).astype(BF)
            keys = jnp.concatenate(
                [kv_all[k, 0, band_rows(b), cut] for k in range(per_window)], axis=0
            )
            values = jnp.concatenate(
                [kv_all[k, 1, band_rows(b), cut] for k in range(per_window)], axis=0
            )
            scores = lax.dot_general(both, keys, LAST, preferred_element_type=F32)
            expo = jnp.exp(scores)
            total = jnp.sum(expo, axis=-1, keepdims=True)
            got = jnp.dot(expo.astype(BF), values, preferred_element_type=F32) / total
            got = jnp.where(lane, got[:band], got[band:]).astype(BF)
            back[1 - mine, band_rows(b), cut] = got
        back_copy(b).start()
        return carry

    def project_attend(b, carry):
        project(b, 0)
        attend(b - 1, 0)
        return carry

    def go_home(j, carry):
        b = lax.rem(j + 1, bands)

        @pl.when(j == 0)
        def _():
            back_copy(0).wait_recv()

        @pl.when(j < bands - 1)
        def _():
            back_copy(b).wait_recv()

        earlier = lax.rem(b + bands - 1, bands)
        near = jnp.concatenate(
            [back[k, band_rows(at), :] for k in range(2) for at in (earlier, b)], axis=0
        )
        home_all[0, band_rows(b), :] = jnp.dot(
            to_home, near, preferred_element_type=F32
        ).astype(BF)
        for r in range(1, n_row):
            home_copy(b, r).start()
        return carry

    def mix(j, carry):
        b = lax.rem(j + 1, bands)
        slot = lax.rem(row - b // steps + n_row, n_row)
        part = pl.ds(pl.multiple_of(lax.rem(b, steps) * chunk, chunk), chunk)
        total = None
        for r in range(n_row):
            if r > 0:
                home_copy(b, r).wait_recv()
            term = lax.dot_general(
                home_all[r, band_rows(b), :], o_all[r], LAST, preferred_element_type=F32
            )
            total = term if total is None else total + term
        base = sphere_all[slot, part, :].astype(F32)
        value = to_sphere(base + attn_rate[...] * (to_sphere(total) - base))
        mixed_all[slot, part, :] = value.astype(BF)
        return carry

    tile = min(512, hidden)

    def raise_slot(r):
        def raise_tile(i, carry):
            cut = pl.ds(pl.multiple_of(i * tile, tile), tile)
            raised = jnp.dot(mixed_all[r], u_full[:, cut], preferred_element_type=F32)
            raised = raised * hidden_gain[:, cut]
            active[r, :, cut] = (
                0.5 * raised * (1.0 + lax.erf(raised * (1.0 / math.sqrt(2.0))))
            ).astype(BF)
            return carry

        lax.fori_loop(0, hidden // tile, raise_tile, 0)

    span = 4 * share
    lowered = []

    def lower_to(r, t):
        z = lax.rem(links.z - links.turn(t) + nz, nz)
        weight = d_full[pl.ds(pl.multiple_of(z * span, span), span), :]
        return z, lax.dot_general(active[r], weight, LAST, preferred_element_type=F32)

    def lower(t):
        d_a.arrive(t)
        d_b.arrive(t)
        for r in range(1, n_row):
            z, got = lower_to(r, t)
            down_send[r, z] = got.astype(BF)
            lowered.append(
                links.send(
                    down_send.at[r, z], down_recv.at[r, z], links.other_row(n_row - r)
                )
            )

    def lower_own(t):
        z, got = lower_to(0, t)
        down_own[z] = got

    def to_neighbour():
        for i in range(steps):
            part = slice(i * chunk, (i + 1) * chunk)
            value = to_sphere(tok[part, :].astype(F32)).astype(BF)
            sphere_all[0, part, :] = value
            piece[mine, part, :] = value

    for copy in local[:3]:
        copy.wait()
    local[4].wait()
    o_a.begin_z()
    local[6].wait()
    d_a.begin_y()
    q_a.begin_z()
    q_a.begin_y()
    local[3].wait()
    to_neighbour()
    for i in early:
        halo[i].start()
    q_b.begin_y()
    o_a.begin_y()
    local[5].wait()
    u_b.begin_y()
    around = [
        links.send(sphere_all.at[0], sphere_all.at[r], links.other_row(r))
        for r in range(1, n_row)
    ]
    shift_columns(inside, early)
    q_a.along(2)
    q_b.begin_z()
    q_a.pass_on()
    o_a.along(2)
    q_a.along(1)
    o_a.along(1)
    u_a.begin_y()
    for t in range(3, nz):
        o_a.along(t)
    q_a.across(2)
    for i in late:
        halo[i].start()
    u_b.begin_z()
    o_a.pass_on()
    shift_columns(inside, late)
    o_a.across(2)
    o_a.across(1)
    q_a.across(1)
    q_b.along(2)
    q_b.along(1)
    for t in range(3, nz):
        q_a.along(t)
    shift_columns(outside, early)
    for t in range(3, nz):
        q_b.along(t)
    u_b.along(2)
    q_b.pass_on()
    shift_columns(outside, late)
    u_a.begin_z()
    d_b.begin_y()
    u_b.along(1)
    q_b.across(1)
    u_a.along(2)
    q_b.across(2)
    for t in range(3, nz):
        q_a.across(t)
    for t in range(3, nz):
        u_b.along(t)
    u_a.pass_on()
    d_a.begin_z()
    for t in range(3, nz):
        q_b.across(t)
    for sent in spread:
        for copy in sent:
            copy.wait_recv()
    for copy in local[7:]:
        copy.wait()
    q_a.arrive_all()
    q_b.arrive_all()
    for t in range(3, nz):
        o_a.across(t)
    project(0, 0)
    lax.fori_loop(1, bands, project_attend, 0)
    attend(bands - 1, 0)
    u_b.pass_on()
    o_a.beyond()
    u_b.across(2)
    for t in range(3, nz):
        u_a.along(t)
    u_a.along(1)
    u_b.across(1)
    d_b.begin_z()
    for copy in around:
        copy.wait_recv()
    lax.fori_loop(0, bands, go_home, 0)
    u_a.across(1)
    d_b.along(2)
    u_a.across(2)
    o_a.arrive_all()
    for t in range(3, nz):
        u_b.across(t)
    for t in range(3, nz):
        u_a.across(t)
    d_a.along(2)
    d_b.pass_on()
    d_a.pass_on()
    lax.fori_loop(0, bands, mix, 0)
    d_b.along(1)
    d_b.across(2)
    for t in range(3, nz):
        d_b.along(t)
    u_a.arrive_all()
    u_b.arrive_all()
    for r in range(1, n_row):
        raise_slot(r)
    d_a.along(1)
    lower(0)
    for t in range(3, nz):
        d_a.along(t)
    d_a.across(2)
    lower(2)
    d_b.across(1)
    d_a.across(1)
    for t in range(3, nz):
        d_a.across(t)
    for t in range(3, nz):
        d_b.across(t)
    lower(1)
    for t in range(3, nz):
        lower(t)
    raise_slot(0)
    lower_own(0)
    lower_own(2)
    for t in [1] + list(range(3, nz)):
        lower_own(t)
    for copy in lowered:
        copy.wait_recv()
    for i in range(steps):
        part = slice(i * chunk, (i + 1) * chunk)
        pieces = []
        for z in range(nz):
            total = down_own[z, part, :]
            for r in range(1, n_row):
                total = total + down_recv[r, z, part, :].astype(F32)
            pieces.append(total)
        base = mixed_all[0, part, :].astype(F32)
        total = to_sphere(jnp.concatenate(pieces, axis=1))
        out[part, :] = to_sphere(base + mlp_rate[...] * (total - base)).astype(BF)
    for copy, when in links.started:
        if when is None:
            copy.wait_send()
        else:
            pl.when(when)(copy.wait_send)

    def drain(b, carry):
        for k in range(1, per_window):
            kv_copy(b, k).wait_send()
        back_copy(b).wait_send()
        for r in range(1, n_row):
            home_copy(b, r).wait_send()
        return carry

    lax.fori_loop(0, bands, drain, 0)


def on_device(
    tokens,
    shifts,
    qkv_weight,
    out_weight,
    up_weight,
    down_weight,
    qk_gain,
    attn_rate,
    mlp_rate,
    hidden_gain,
):
    n_row = lax.axis_size("row")
    n_col = lax.axis_size("col")
    local_rows, cols, depth = tokens.shape
    width = qkv_weight.shape[2]
    hidden = up_weight.shape[1]
    own = local_rows * cols
    rows = local_rows * n_row
    count = rows * cols
    bands = rows // WIN
    per_window = WIN // cols
    share = depth // n_col
    nz = n_col // 4
    span = 4 * share
    steps = own // (WIN * cols)
    copies = 7 * (4 * nz + 2) + steps * n_row + (n_row - 1) * (5 * nz + 1)
    dma = pltpu.SemaphoreType.DMA
    dims = (local_rows, cols, depth, width, hidden)
    room = 67043328 - own * depth * 2 - 2048

    def layer(side, *operands):
        return pl.pallas_call(
        functools.partial(layer_kernel, n_row, n_col, dims, side),
        out_shape=jax.ShapeDtypeStruct((own, depth), BF),
        in_specs=[SMEM] + [HBM] * 9,
        out_specs=VMEM,
        scratch_shapes=[
            pltpu.VMEM((depth, 3 * width), BF),
            pltpu.VMEM((n_row, depth, width), BF),
            pltpu.VMEM((depth, hidden), BF),
            pltpu.VMEM((depth, hidden), BF),
            pltpu.VMEM((own, depth), BF),
            pltpu.VMEM((2, own, depth), BF),
            pltpu.VMEM((n_row, own, depth), BF),
            pltpu.VMEM((n_row, own, depth), BF),
            pltpu.VMEM((count, width), BF),
            pltpu.VMEM((per_window, 2, count, width), BF),
            pltpu.VMEM((2, count, width), BF),
            pltpu.VMEM((n_row, count, width), BF),
            pltpu.VMEM((n_row, own, depth), BF),
            pltpu.VMEM((n_row, own, hidden), BF),
            pltpu.VMEM((n_row, nz, own, span), BF),
            pltpu.VMEM((n_row, nz, own, span), BF),
            pltpu.VMEM((nz, own, span), F32),
            dma((11,)),
            dma((copies,)),
            dma((copies,)),
            dma((bands, per_window)),
            dma((bands, per_window)),
            dma((bands,)),
            dma((bands,)),
            dma((bands, n_row)),
            dma((bands, n_row)),
            pltpu.VMEM((1, width), F32),
            pltpu.VMEM((1, depth), F32),
            pltpu.VMEM((1, depth), F32),
            pltpu.VMEM((1, hidden), F32),
        ],
        compiler_params=pltpu.CompilerParams(
            collective_id=0 if side > 0 else 1, has_side_effects=True, vmem_limit_bytes=room
        ),
        name="layer",
    )(*operands)

    result = lax.cond(
        shifts[1] < cols,
        functools.partial(layer, 1),
        functools.partial(layer, -1),
        shifts,
        tokens.reshape(own, depth),
        qkv_weight.transpose(1, 0, 2),
        out_weight.T,
        up_weight,
        down_weight.T,
        qk_gain.reshape(1, width),
        attn_rate.reshape(1, depth),
        mlp_rate.reshape(1, depth),
        hidden_gain.reshape(1, hidden),
    )
    return result.reshape(local_rows, cols, depth)


def solution(mesh):
    return jax.shard_map(
        on_device,
        mesh=mesh,
        in_specs=(
            P("row", "col", None),
            P(),
            P("col", None, "row"),
            P("row", "col"),
            P("col", "row"),
            P("row", "col"),
            P("row"),
            P(),
            P(),
            P("row"),
        ),
        out_specs=P("row", "col", None),
        check_vma=False,
    )
```
